512 devices in a mesh: groups: 2 (over y), ep: 64 (over z, core), tp: 4 (over x).
Axes of the slice: x: 4, y: 2, z: 32, core: 2. Of those that a mesh axis runs over, the one named last changes fastest.
The devices are a block of a 4x8x32 slice.
Arguments:
- hidden: bfloat16 [8192, 2880], P(('groups', 'ep')), parts along dimension 0, may hold values from -6 to 6
- route_experts: int32 [8192, 4], P(('groups', 'ep')), parts along dimension 0, may hold values from 0 to 63, all different within a row; in each aligned block of 64 rows (0 to 63, 64 to 127, ...) at most 8 rows name the same one
- route_weight: float32 [8192, 4], P(('groups', 'ep')), parts along dimension 0, may hold values from 0.1 to 0.6
- norm_gain: bfloat16 [2880], replicated, may hold values from 0.099609375 to 1.8984375
- gate_up_codes: int32 [64, 360, 5120], P('ep', None, 'tp'), may hold values from -2147483648 to 2147483646
- gate_up_scales: bfloat16 [64, 90, 5120], P('ep', None, 'tp'), as said below
- gate_up_bias: bfloat16 [64, 5120], P('ep', 'tp'), may hold values from -3 to 3
- down_codes: int32 [64, 2560, 360], P('ep', 'tp'), may hold values from -2147483648 to 2147483646
- down_scales: bfloat16 [64, 80, 2880], P('ep', 'tp'), as said below
- down_bias: bfloat16 [64, 2880], P('ep', 'tp'), may hold values from -3 to 3
Outputs:
- layer_out: bfloat16 [8192, 2880], P(('groups', 'ep'), 'tp'), parts along dimension 0
The draws below stay inside these ranges and needn't reach their ends.
There are 2 independent parts, one for each index of `groups`. The reference program is written for one: setup_inputs(seed, part) draws one part's arguments, and reference() takes and returns one part's arrays. A program takes and returns all parts, laid end to end along the dimension named above; an argument that names none is the same for every part. Nothing has to cross between parts.
Inputs may be any that keep to these rules, and one draw needn't show every extreme that they name: `route_experts`: each row names 4 different experts. In each aligned block of 64 rows no expert is named by more than 8 rows, and in some blocks one expert is named by exactly 8 rows. `gate_up_scales`: every scale is a power of two. `down_scales`: every scale is a power of two.
All inputs are finite; a program needn't handle non-finite values.
Results may differ from the reference program's by a relative error of at most 0.013.
Values may be sent and summed in bfloat16 or wider, within the bound.
A program may use at most 128 MiB of HBM per device.

```python
import math
import jax
import jax.numpy as jnp
import numpy as np
from jax import lax

D = 2880
TOP = 4
FF = 2560
TOK_EP = 64
EXPERTS = 64
TOKENS = 4096
CAP = 8
N_EP = 64
N_TP = 4


def draw_gate_up_scales(key, part):
    centre = int(math.floor(math.log2(0.5 / math.sqrt(D))))
    powers = jax.random.randint(jax.random.fold_in(key, 11), (EXPERTS, D // 32, 2 * FF), centre - 1, centre + 2)
    return jnp.exp2(powers.astype(jnp.float32)).astype(jnp.bfloat16)


def draw_down_scales(key, part):
    centre = int(math.floor(math.log2(0.5 / math.sqrt(FF))))
    powers = jax.random.randint(jax.random.fold_in(key, 23), (EXPERTS, FF // 32, D), centre - 1, centre + 2)
    return jnp.exp2(powers.astype(jnp.float32)).astype(jnp.bfloat16)


def place_ends(entries, stream_key, smallest, largest):
    extent = entries.shape
    index_at = [jax.random.randint(jax.random.fold_in(stream_key, axis), (), 0, extent[axis]) for axis in range(len(extent))]
    entries = entries.at[tuple(index_at)].set(smallest)
    longest = extent.index(max(extent))
    index_at[longest] = (index_at[longest] + 1) % extent[longest]
    return entries.at[tuple(index_at)].set(largest)


def shard_levels(own_key, extent, cuts, low, high):
    def one(axis_at, blocks):
        heights = jax.random.uniform(jax.random.fold_in(jax.random.fold_in(own_key, 6), axis_at), (blocks,), jnp.float32, low / len(cuts), high / len(cuts))
        return jnp.repeat(jnp.exp(heights), extent[axis_at] // blocks).reshape((-1,) + (1,) * (len(extent) - axis_at - 1))

    level = one(*cuts[0])
    for cut in cuts[1:]:
        level = level * one(*cut)
    return level


def shared_out(rng, own, number, rows, amount, top, reach, slope):
    ranking = jax.random.permutation(rng, amount)
    crowded, common = load_shares(amount, rows * top, reach, slope, True), load_shares(amount, rows * top, reach, slope, False)
    places = jnp.arange(amount)

    def named(lengths, offset_by):
        used = int((lengths > 0).sum())
        fixed = max(1, used // 4)
        moved = fixed + (places - fixed + offset_by * (used - fixed)) % max(1, amount - fixed)
        return jnp.zeros((amount,), jnp.int32).at[ranking[jnp.where(places < fixed, places, moved)]].set(jnp.asarray(lengths, jnp.int32))

    lengths = jnp.where(number % 4 == 0, named(crowded, number // 4), named(common, number - number // 4 - 1))
    mixed = jax.random.permutation(jax.random.fold_in(own, 3), amount)
    giver, taker = mixed[0:amount // 2 * 2:2], mixed[1:amount // 2 * 2:2]
    margin = jnp.minimum(lengths[giver] - 1, reach - lengths[taker]) // 2
    margin = jnp.where((giver == ranking[0]) | (taker == ranking[0]) | (lengths[taker] == 0), 0, jnp.maximum(margin, 0))
    moved = jax.random.randint(jax.random.fold_in(own, 4), (amount // 2,), 0, 1 << 20) % (margin + 1)
    lengths = lengths.at[giver].add(-moved).at[taker].add(moved)
    items = jnp.searchsorted(jnp.cumsum(lengths), jnp.arange(rows * top), side="right").astype(jnp.int32)
    grid = items.reshape(top, rows).T
    grid = grid[jax.random.permutation(jax.random.fold_in(own, 1), rows)]
    offset_by = jax.random.randint(jax.random.fold_in(own, 2), (rows, 1), 0, top)
    return jnp.take_along_axis(grid, (jnp.arange(top)[None, :] + offset_by) % top, axis=1)


def load_shares(number_of, total, reach, skew, full):
    portions = [(1 << 20) // math.isqrt(standing ** skew) + 1 for standing in range(1, number_of + 1)]
    largest = reach if full else min(reach, max(-(-total // number_of), total * portions[0] // sum(portions)))
    least = 1 if total - largest >= number_of - 1 else 0
    holding, surplus = [largest] + [least] * (number_of - 1), total - largest - least * (number_of - 1)
    while surplus > 0:
        free = [i for i in range(1, number_of) if holding[i] < largest] or [i for i in range(1, number_of) if holding[i] < reach]
        whole, budget = sum([portions[i] for i in free]), surplus
        for i in free:
            extra = min(reach - holding[i], max(1, budget * portions[i] // whole), surplus)
            holding[i] = holding[i] + extra
            surplus = surplus - extra
    return np.array(holding)


def bell_draw(rng, extent, spread, reach, shards=(), held_as=jnp.bfloat16):
    gain = shard_levels(rng, extent, shards, -0.22, 0.18) if shards else 1.0
    entries = jax.random.normal(rng, extent, jnp.float32) * spread * gain
    return jnp.minimum(jnp.maximum(entries, -reach), reach).astype(held_as)


def setup_inputs(seed: int = 0, part: int = 0) -> dict:
    key_of = jax.random.split(jax.random.key(seed), 11)
    part_splits = jax.random.split(jax.random.fold_in(key_of[10], part), 11)
    hidden = bell_draw(part_splits[0], (TOKENS, D), 1.0, 6.0, ((0, 64),))
    route_experts_keys = jax.random.split(jax.random.fold_in(part_splits[1], 1), TOKENS // TOK_EP)
    route_experts_turns = jax.random.permutation(jax.random.fold_in(part_splits[1], 3), TOKENS // TOK_EP)
    route_experts = jax.vmap(lambda own, number: shared_out(jax.random.fold_in(part_splits[1], 2), own, number, TOK_EP, EXPERTS, TOP, CAP, 2))(route_experts_keys, route_experts_turns).reshape((TOKENS, TOP))
    route_weight = jnp.clip(0.1 + 0.5 * jax.random.uniform(part_splits[2], (TOKENS, TOP), jnp.float32) ** shard_levels(part_splits[2], (TOKENS, TOP), ((0, 64),), -0.2, 0.2), 0.1, 0.6)
    norm_gain = jnp.clip(1.0 + 0.18 * jax.random.normal(key_of[3], (D,), jnp.float32), 0.099609375, 1.8984375).astype(jnp.bfloat16)
    gate_up_codes = place_ends(jax.random.randint(key_of[4], (EXPERTS, D // 8, 2 * FF), -2147483648, 2147483647), jax.random.fold_in(key_of[4], 1), -2147483648, 2147483646).astype(jnp.int32)
    gate_up_scales = draw_gate_up_scales(jax.random.fold_in(key_of[10], 71), part)
    gate_up_bias = bell_draw(key_of[6], (EXPERTS, 2 * FF), 0.5, 3.0, ((0, 64), (1, 4)))
    down_codes = place_ends(jax.random.randint(key_of[7], (EXPERTS, FF, D // 8), -2147483648, 2147483647), jax.random.fold_in(key_of[7], 1), -2147483648, 2147483646).astype(jnp.int32)
    down_scales = draw_down_scales(jax.random.fold_in(key_of[10], 71), part)
    down_bias = bell_draw(key_of[9], (EXPERTS, D), 0.5, 3.0, ((0, 64), (1, 4)))
    return {"hidden": hidden, "route_experts": route_experts, "route_weight": route_weight, "norm_gain": norm_gain, "gate_up_codes": gate_up_codes, "gate_up_scales": gate_up_scales, "gate_up_bias": gate_up_bias, "down_codes": down_codes, "down_scales": down_scales, "down_bias": down_bias}


def decode_nibble(nibble):
    magnit = nibble & 7
    exponent = jnp.maximum(jnp.right_shift(magnit, 1) - 1, 0)
    doubled = jnp.where(magnit < 2, magnit, jnp.left_shift(2 + (magnit & 1), exponent))
    signed_val = doubled.astype(jnp.float32) * 0.5
    return jnp.where(nibble >= 8, -signed_val, signed_val)

def unpack_weights(packed, scaling):
    row_count = packed.shape[0]
    shifts = jnp.arange(8, dtype=jnp.int32) * 4
    nibble = jnp.right_shift(packed[:, :, None], shifts[None, None, :]) & 15
    nibble = nibble.reshape(row_count, packed.shape[1] * 8)
    signed_val = decode_nibble(nibble)
    signed_val = signed_val.reshape(row_count // 32, 32, -1) * scaling.astype(jnp.float32)[:, None, :]
    return signed_val.reshape(row_count, -1).astype(jnp.bfloat16)

def unpack_rows(packed, scaling):
    row_count = packed.shape[0] * 8
    shifts = jnp.arange(8, dtype=jnp.int32) * 4
    nibble = jnp.right_shift(packed[:, None, :], shifts[None, :, None]) & 15
    nibble = nibble.reshape(row_count, packed.shape[1])
    signed_val = decode_nibble(nibble)
    signed_val = signed_val.reshape(row_count // 32, 32, -1) * scaling.astype(jnp.float32)[:, None, :]
    return signed_val.reshape(row_count, -1).astype(jnp.bfloat16)

def rms_normed(hidden, norm_gain):
    widened = hidden.astype(jnp.float32)
    mean_square = lax.optimization_barrier(jnp.mean(widened * widened, axis=-1, keepdims=True))
    scaled = widened * lax.rsqrt(mean_square + 1e-05) * norm_gain.astype(jnp.float32)
    return scaled.astype(jnp.bfloat16)

def slot_numbers(routes):
    block_count, row_count, top_count = routes.shape
    flat_routes = routes.reshape(block_count, row_count * top_count)
    onehot = (flat_routes[:, :, None] == jnp.arange(EXPERTS, dtype=jnp.int32)[None, None, :]).astype(jnp.int32)
    before = jnp.cumsum(onehot, axis=1) - onehot
    slot_of = lax.optimization_barrier(jnp.sum(before * onehot, axis=2))
    return slot_of.reshape(block_count, row_count, top_count)

def expert_rows(normed_rows, gate_codes, gate_scales, gate_bias, lower_codes, lower_scales, lower_bias):
    gate_up_weight = unpack_rows(gate_codes, gate_scales)
    down_weight = unpack_weights(lower_codes, lower_scales)
    projected = jnp.dot(normed_rows, gate_up_weight, preferred_element_type=jnp.float32) + gate_bias.astype(jnp.float32)
    gate_part = jnp.minimum(projected[:, 0::2], 7.0)
    upward = jnp.clip(projected[:, 1::2], -7.0, 7.0)
    activated = (gate_part * jax.nn.sigmoid(1.702 * gate_part) * (upward + 1.0)).astype(jnp.bfloat16)
    quarter = FF // N_TP
    summed = jnp.zeros((normed_rows.shape[0], D), jnp.float32)
    for tp_part in range(N_TP):
        partial_value = jnp.dot(activated[:, tp_part * quarter:(tp_part + 1) * quarter], down_weight[tp_part * quarter:(tp_part + 1) * quarter], preferred_element_type=jnp.float32).astype(jnp.bfloat16)
        summed = summed + partial_value.astype(jnp.float32)
    return (summed + lower_bias.astype(jnp.float32)).astype(jnp.bfloat16)

def reference(hidden, route_experts, route_weight, norm_gain, gate_up_codes, gate_up_scales, gate_up_bias, down_codes, down_scales, down_bias):
    normed = rms_normed(hidden, norm_gain)
    routes = route_experts.reshape(N_EP, TOK_EP, TOP)
    slot_of = slot_numbers(routes)
    token_ids = jnp.broadcast_to(jnp.arange(TOKENS, dtype=jnp.int32).reshape(N_EP, TOK_EP, 1), routes.shape)
    block_ids = jnp.broadcast_to(jnp.arange(N_EP, dtype=jnp.int32).reshape(N_EP, 1, 1), routes.shape)
    slot_table = jnp.zeros((EXPERTS, N_EP, CAP), jnp.int32).at[routes, block_ids, slot_of].set(token_ids)

    def one_expert(expert):
        picked = normed[slot_table[expert].reshape(-1)]
        return expert_rows(picked, gate_up_codes[expert], gate_up_scales[expert], gate_up_bias[expert], down_codes[expert], down_scales[expert], down_bias[expert])
    outputs = lax.map(one_expert, jnp.arange(EXPERTS, dtype=jnp.int32)).reshape(EXPERTS, N_EP, CAP, D)
    weights = route_weight.reshape(N_EP, TOK_EP, TOP)
    running = hidden.astype(jnp.float32).reshape(N_EP, TOK_EP, D)
    for position in range(TOP):
        fetched = outputs[routes[:, :, position], block_ids[:, :, position], slot_of[:, :, position]]
        running = running + weights[:, :, position][:, :, None] * fetched.astype(jnp.float32)
    return running.reshape(TOKENS, D).astype(jnp.bfloat16)
```

```python
import functools

import jax
import jax.numpy as jnp
from jax import lax
from jax.experimental import pallas as pl
from jax.experimental.pallas import tpu as pltpu
from jax.sharding import PartitionSpec as P

CAP = 8
CHUNKS = 2
F32 = jnp.float32
BF16 = jnp.bfloat16


def dot(a, b):
    return jnp.dot(a, b, preferred_element_type=F32)


def iota(shape, dim):
    return lax.broadcasted_iota(jnp.int32, shape, dim)


def neighbours(ep, tp):
    me = lax.axis_index("ep")
    core = lax.rem(me, 2)
    col = lax.axis_index("tp")
    return dict(
        me=me,
        up=lax.rem(me + 2, ep),
        down=lax.rem(me + ep - 2, ep),
        pal=me + 1 - 2 * core,
        col=col,
        right=lax.rem(col + 1, tp),
        left=lax.rem(col + tp - 1, tp),
        across=lax.rem(col + 2, tp),
    )


def greet(at):
    barrier = pltpu.get_barrier_semaphore()
    for place in ({"ep": at["up"]}, {"ep": at["down"]}, {"ep": at["pal"]}, {"tp": at["right"]}, {"tp": at["left"]}):
        pl.semaphore_signal(barrier, inc=1, device_id=place, device_id_type=pl.DeviceIdType.MESH)
    pl.semaphore_wait(barrier, 5)


def remote(src, dst, send, recv, place):
    return pltpu.make_async_remote_copy(
        src_ref=src, dst_ref=dst, send_sem=send, recv_sem=recv, device_id=place, device_id_type=pl.DeviceIdType.MESH
    )


def dispatch_kernel(
    ep, tp, top, meta_at, block_ref, rows_ref, mix_ref, held, handed, own_sem, zs, zr, ds, dr, xs, xr
):
    pairs = held.shape[0]
    tokens = held.shape[2]
    part = tokens // CHUNKS
    at = neighbours(ep, tp)
    greet(at)
    first = pltpu.make_async_copy(block_ref, held.at[0, 0], own_sem)
    first.start()
    first.wait()

    def piece(pair, side, h):
        return held.at[pair, side, pl.ds(h * part, part)]

    def hop(s, side, h):
        src = piece(0, 0, h) if isinstance(s, int) and s == 1 else piece(s - 1, side, h)
        place = {"ep": at["up"] if side == 0 else at["down"]}
        return remote(src, piece(s, side, h), zs.at[s, side, h], zr.at[s, side, h], place)

    def last_hop(side, h):
        place = {"ep": at["up"] if side == 0 else at["down"]}
        return remote(
            piece(pairs - 1, side, h), piece(0, 1, h), zs.at[0, side, h], zr.at[0, side, h], place
        )

    def last_side(h):
        return 0 if h < CHUNKS // 2 else 1

    def tile(col, pair, p):
        return rows_ref.at[col, pair * 2 + p]

    def to_pal(pair):
        return remote(
            handed.at[pair], tile(at["col"], pair, 1), ds.at[pair], dr.at[pair], {"ep": at["pal"]}
        )

    def across_right(pair, p):
        return remote(
            tile(at["col"], pair, p), tile(at["col"], pair, p), xs.at[pair * 2 + p, 0],
            xr.at[pair * 2 + p, 0], {"tp": at["right"]},
        )

    def across_left(pair, p):
        return remote(
            tile(at["col"], pair, p), tile(at["col"], pair, p), xs.at[pair * 2 + p, 1],
            xr.at[pair * 2 + p, 1], {"tp": at["left"]},
        )

    def from_left(pair, p):
        return remote(
            tile(at["left"], pair, p), tile(at["left"], pair, p), xs.at[pair * 2 + p, 0],
            xr.at[pair * 2 + p, 0], {"tp": at["right"]},
        )

    def from_right(pair, p):
        return remote(
            tile(at["right"], pair, p), tile(at["right"], pair, p), xs.at[pair * 2 + p, 1],
            xr.at[pair * 2 + p, 1], {"tp": at["left"]},
        )

    def relay(pair, p):
        col, place = (at["left"], at["right"]) if p == 0 else (at["right"], at["left"])
        return remote(
            tile(col, pair, p), tile(col, pair, p), xs.at[pair * 2 + p, 2], xr.at[pair * 2 + p, 2],
            {"tp": place},
        )

    def relayed(pair, p):
        return remote(
            tile(at["across"], pair, p), tile(at["across"], pair, p), xs.at[pair * 2 + p, 2],
            xr.at[pair * 2 + p, 2], {"tp": at["right"]},
        )

    for h in range(CHUNKS):
        for side in range(2):
            hop(1, side, h).start()

    both = 2 * tokens
    lane = iota((both, 128), 1)
    ks, ls = iota((128, 128), 0), iota((128, 128), 1)
    own_cols = (ls < 16).astype(BF16)
    pal_cols = ((ls >= 16) & (ls < 32)).astype(BF16)
    ti, tj = iota((both, both), 0), iota((both, both), 1)
    earlier = ((tj < ti) & ((ti < tokens) == (tj < tokens))).astype(BF16)
    wanted = lax.rem(lane, 16) - jnp.where(iota((both, 128), 0) >= tokens, 8, 0)
    wanted = wanted.astype(F32)
    id_lanes = (lane >= meta_at) & (lane < meta_at + top)
    own_id = at["me"].astype(F32)
    pal_id = at["pal"].astype(F32)

    def select(pair):
        width = held.shape[3]
        block = held[pair].reshape(both, width)
        meta = block[:, width - 128 :].astype(F32)
        weights = pltpu.roll(meta, 128 - top, axis=1)
        is_own = id_lanes & (meta == own_id)
        is_pal = id_lanes & (meta == pal_id)
        match = dot(jnp.where(is_own, 1.0, 0.0).astype(BF16), own_cols) + dot(
            jnp.where(is_pal, 1.0, 0.0).astype(BF16), pal_cols
        )
        weight = dot(jnp.where(is_own, weights, 0.0).astype(BF16), own_cols) + dot(
            jnp.where(is_pal, weights, 0.0).astype(BF16), pal_cols
        )
        slot = dot(earlier, match.astype(BF16))
        placed = (match > 0.5) & (slot == wanted)
        mix_ref[pair] = jnp.where(placed, weight, 0.0).astype(BF16)
        pick = jnp.transpose(jnp.where(placed, 1.0, 0.0))[:32].astype(BF16)
        picked = dot(pick, block).astype(BF16)
        rows_ref[at["col"], pair * 2] = picked[:16]
        handed[pair] = picked[16:]

    def body(u, carry):
        @pl.when(u < pairs - 1)
        def _():
            s = u + 1
            for h in range(CHUNKS):
                for side in range(2):
                    hop(s, side, h).wait_recv()

                    @pl.when(s < pairs - 1)
                    def _():
                        hop(s + 1, side, h).start()

                    if side == last_side(h):

                        @pl.when(s == pairs - 1)
                        def _():
                            last_hop(side, h).start()

        @pl.when(u == pairs - 1)
        def _():
            for h in range(CHUNKS):
                last_hop(last_side(h), h).wait_recv()

        @pl.when(u < pairs)
        def _():
            pair = lax.rem(u + 1, pairs)
            select(pair)
            to_pal(pair).start()
            across_right(pair, 0).start()
            across_left(pair, 0).start()

        @pl.when((u >= 1) & (u < pairs + 1))
        def _():
            pair = lax.rem(u, pairs)
            to_pal(pair).wait_recv()
            across_right(pair, 1).start()
            across_left(pair, 1).start()
            from_left(pair, 0).wait_recv()
            relay(pair, 0).start()

        @pl.when(u >= 2)
        def _():
            pair = lax.rem(u - 1, pairs)
            from_right(pair, 1).wait_recv()
            relay(pair, 1).start()

        return carry

    lax.fori_loop(0, pairs + 2, body, 0)

    def finish(pair, carry):
        from_right(pair, 0).wait_recv()
        from_left(pair, 1).wait_recv()
        to_pal(pair).wait_send()
        for p in range(2):
            relayed(pair, p).wait_recv()
            across_right(pair, p).wait_send()
            across_left(pair, p).wait_send()
            relay(pair, p).wait_send()
        return carry

    lax.fori_loop(0, pairs, finish, 0)

    def sent(s, carry):
        for h in range(CHUNKS):
            for side in range(2):
                hop(s, side, h).wait_send()
        return carry

    lax.fori_loop(1, pairs, sent, 0)
    for h in range(CHUNKS):
        last_hop(last_side(h), h).wait_send()


def dispatch(block, ep, tp, top, meta_at):
    tokens, width = block.shape
    pairs = ep // 4
    dma = pltpu.SemaphoreType.DMA
    vmem = pl.BlockSpec(memory_space=pltpu.VMEM)
    return pl.pallas_call(
        functools.partial(dispatch_kernel, ep, tp, top, meta_at),
        out_shape=(
            jax.ShapeDtypeStruct((tp, 2 * pairs, 16, width), BF16),
            jax.ShapeDtypeStruct((pairs, 2 * tokens, 128), BF16),
        ),
        in_specs=[pl.BlockSpec(memory_space=pl.ANY)],
        out_specs=(vmem, vmem),
        scratch_shapes=[
            pltpu.VMEM((pairs, 2, tokens, width), BF16),
            pltpu.VMEM((pairs, 16, width), BF16),
            dma(()),
            dma((pairs, 2, CHUNKS)),
            dma((pairs, 2, CHUNKS)),
            dma((pairs,)),
            dma((pairs,)),
            dma((2 * pairs, 3)),
            dma((2 * pairs, 3)),
        ],
        compiler_params=pltpu.CompilerParams(
            collective_id=0, has_side_effects=True, vmem_limit_bytes=40 << 20
        ),
        name="dispatch",
    )(block)


def nibble_value(word, shift):
    top_bits = lax.shift_left(word, 28 - shift)
    magnit = lax.shift_right_logical(top_bits, 28) & 7
    doubled = magnit + jnp.maximum(magnit - 4, 0) + 2 * jnp.maximum(magnit - 6, 0)
    value = doubled.astype(F32)
    return jnp.where(top_bits < 0, -value, value)


def experts_kernel(
    rows_ref, codes_ref, scales_ref, bias_ref, low_codes_ref, low_scales_ref, out_ref, upper, lower, act, spread
):
    tp = rows_ref.shape[0]
    width = rows_ref.shape[2]
    columns = codes_ref.shape[1]
    units = upper.shape[0] // tp
    real_units = codes_ref.shape[0] // 2 // tp
    hidden_units = lower.shape[1]
    for q in range(tp):
        upper[q * units + real_units : (q + 1) * units] = jnp.zeros(
            (units - real_units, 16, columns), BF16
        )

    shift = 4 * iota((8, 8, columns), 1)

    def decode(u, carry):
        words = codes_ref[pl.ds(pl.multiple_of(u * 8, 8), 8), :]
        value = nibble_value(jnp.broadcast_to(words[:, None, :], (8, 8, columns)), shift)
        value = value.reshape(2, 32, columns) * (0.5 * scales_ref[u])[:, None, :]
        value = value.reshape(4, 16, columns).astype(BF16)
        for k in range(4):
            unit = 4 * u + k
            upper[unit + (units - real_units) * (unit // real_units)] = value[k]
        return carry

    lax.fori_loop(0, codes_ref.shape[0] // 8, decode, 0)

    word, lanes = iota((128, width), 0), iota((128, width), 1)
    for j in range(8):
        spread[j * 128 : (j + 1) * 128] = (lanes == 8 * word + j).astype(BF16)

    def decode_low(q, carry):
        words = low_codes_ref[:, pl.ds(pl.multiple_of(q * 128, 128), 128)]
        whole = jnp.concatenate([nibble_value(words, 4 * j).astype(BF16) for j in range(8)], axis=1)
        value = dot(whole, spread[...])
        value = value.reshape(hidden_units // 32, 32, width) * (0.5 * low_scales_ref[q])[:, None, :]
        lower[q] = value.reshape(hidden_units, width).astype(BF16)
        return carry

    lax.fori_loop(0, tp, decode_low, 0)

    si, sj = iota((256, 128), 0), iota((256, 128), 1)
    evens = (si == 2 * sj).astype(BF16)

    def project(n, carry):
        at = pl.ds(pl.multiple_of(n * 256, 256), 256)
        total = bias_ref[:, at]
        for q in range(tp):
            weight = upper[q * units : (q + 1) * units, :, at].reshape(units * 16, 256)
            total = total + dot(rows_ref[q], weight)
        gate = jnp.minimum(total, 7.0)
        upward = jnp.clip(pltpu.roll(total, 255, axis=1), -7.0, 7.0)
        value = (gate * jax.nn.sigmoid(1.702 * gate) * (upward + 1.0)).astype(BF16)
        act[:, pl.ds(pl.multiple_of(n * 128, 128), 128)] = dot(value, evens).astype(BF16)
        return carry

    lax.fori_loop(0, columns // 256, project, 0)

    def lower_dot(q, carry):
        out_ref[q] = dot(act[...], lower[q]).astype(BF16)
        return carry

    lax.fori_loop(0, tp, lower_dot, 0)


def experts(rows, codes, scales, bias, low_codes, low_scales):
    tp, row_count, width = rows.shape
    columns = codes.shape[1]
    hidden_units = low_codes.shape[0]
    vmem = pl.BlockSpec(memory_space=pltpu.VMEM)
    return pl.pallas_call(
        experts_kernel,
        out_shape=jax.ShapeDtypeStruct((tp, row_count, width), BF16),
        in_specs=[vmem] * 6,
        out_specs=vmem,
        scratch_shapes=[
            pltpu.VMEM((tp * width // 16, 16, columns), BF16),
            pltpu.VMEM((tp, hidden_units, width), BF16),
            pltpu.VMEM((row_count, hidden_units), BF16),
            pltpu.VMEM((1024, width), BF16),
        ],
        compiler_params=pltpu.CompilerParams(vmem_limit_bytes=56 << 20),
        name="experts",
    )(rows, codes, scales, bias, low_codes, low_scales)


def combine_kernel(
    ep, tp, part_ref, mix_ref, bias_ref, own_ref, out_ref,
    across, summed, staged, direct, outs, handed, moving, leaving, own_sum,
    zs, zr, ds, dr, xs, xr,
):
    pairs = mix_ref.shape[0]
    tokens = moving.shape[2]
    part = tokens // CHUNKS
    at = neighbours(ep, tp)
    greet(at)

    def last_side(h):
        return 1 if h < CHUNKS // 2 else 0

    def up_or_down(side):
        return {"ep": at["up"] if side == 1 else at["down"]}

    def hop(s, side, h):
        src = leaving.at[s, side, pl.ds(h * part, part)]
        dst = moving.at[s - 1, side, pl.ds(h * part, part)]
        return remote(src, dst, zs.at[s - 1, side, h], zr.at[s - 1, side, h], up_or_down(side))

    def first_hop(side, h):
        src = leaving.at[0, 1, pl.ds(h * part, part)]
        dst = moving.at[pairs - 1, side, pl.ds(h * part, part)]
        return remote(src, dst, zs.at[pairs - 1, side, h], zr.at[pairs - 1, side, h], up_or_down(side))

    def far(p):
        return {"tp": at["right"] if p == 0 else at["left"]}

    def near(p):
        return {"tp": at["left"] if p == 0 else at["right"]}

    def two_away(t, p):
        return remote(part_ref.at[at["across"], t], across.at[t], xs.at[t, 0], xr.at[t, 0], far(p))

    def one_away(t, p):
        col = at["left"] if p == 0 else at["right"]
        return remote(part_ref.at[col, t], direct.at[t], xs.at[t, 1], xr.at[t, 1], near(p))

    def onward(t, p):
        return remote(staged.at[t], summed.at[t], xs.at[t, 2], xr.at[t, 2], far(p))

    def to_pal(pair):
        return remote(
            handed.at[pair], outs.at[pair, pl.ds(16, 16)], ds.at[pair], dr.at[pair], {"ep": at["pal"]}
        )

    for h in range(CHUNKS):
        side = 1 - last_side(h)
        moving[pairs - 1, side, h * part : (h + 1) * part] = jnp.zeros((part, moving.shape[3]), BF16)

    def pair_of(u):
        return lax.rem(pairs - u, pairs)

    def body(t, carry):
        @pl.when(t < pairs)
        def _():
            pair = pair_of(t)
            for p in range(2):
                two_away(pair * 2 + p, p).start()
            for p in range(2):
                one_away(pair * 2 + p, p).start()

        @pl.when(t >= 3)
        def _():
            u = t - 3
            pair = pair_of(u)
            to_pal(pair).wait_recv()
            mixed = dot(mix_ref[pair][:, :32], outs[pair])

            @pl.when(u == 0)
            def _():
                own_sum[...] = mixed[:tokens]
                leaving[0, 1] = mixed[tokens:].astype(BF16)
                for h in range(CHUNKS):
                    first_hop(last_side(h), h).start()

            @pl.when(u > 0)
            def _():
                for h in range(CHUNKS):
                    for side in (last_side(h), 1 - last_side(h)):
                        arrival = remote(
                            leaving.at[pair, side, pl.ds(h * part, part)],
                            moving.at[pair, side, pl.ds(h * part, part)],
                            zs.at[pair, side, h],
                            zr.at[pair, side, h],
                            up_or_down(side),
                        )
                        if side == last_side(h):
                            arrival.wait_recv()
                        else:

                            @pl.when(u > 1)
                            def _():
                                arrival.wait_recv()

                        begin = side * tokens + h * part
                        value = mixed[begin : begin + part] + moving[
                            pair, side, h * part : (h + 1) * part
                        ].astype(F32)
                        leaving[pair, side, h * part : (h + 1) * part] = value.astype(BF16)
                        hop(pair, side, h).start()

        @pl.when((t >= 1) & (t < pairs + 1))
        def _():
            pair = pair_of(t - 1)
            for p in range(2):
                tile = pair * 2 + p
                two_away(tile, p).wait_recv()
                col = at["right"] if p == 0 else at["left"]
                staged[tile] = (across[tile].astype(F32) + part_ref[col, tile].astype(F32)).astype(BF16)
                onward(tile, p).start()

        @pl.when((t >= 2) & (t < pairs + 2))
        def _():
            pair = pair_of(t - 2)
            for p in (1, 0):
                tile = pair * 2 + p
                one_away(tile, p).wait_recv()
                onward(tile, p).wait_recv()
                total = (
                    summed[tile].astype(F32)
                    + direct[tile].astype(F32)
                    + part_ref[at["col"], tile].astype(F32)
                    + bias_ref[...]
                ).astype(BF16)
                if p == 1:
                    handed[pair] = total
                    to_pal(pair).start()
                else:
                    outs[pair, :16] = total

        return carry

    lax.fori_loop(0, pairs + 3, body, 0)

    for side in range(2):
        for h in range(CHUNKS):
            hop(1, side, h).wait_recv()
    total = own_ref[...].astype(F32) + own_sum[...] + moving[0, 0].astype(F32) + moving[0, 1].astype(F32)
    out_ref[...] = total[:, : out_ref.shape[1]].astype(BF16)

    def finish(pair, carry):
        to_pal(pair).wait_send()
        for p in range(2):
            two_away(pair * 2 + p, p).wait_send()
            one_away(pair * 2 + p, p).wait_send()
            onward(pair * 2 + p, p).wait_send()
        return carry

    lax.fori_loop(0, pairs, finish, 0)

    def sent(s, carry):
        for h in range(CHUNKS):
            for side in range(2):
                hop(s, side, h).wait_send()
        return carry

    lax.fori_loop(1, pairs, sent, 0)
    for h in range(CHUNKS):
        first_hop(last_side(h), h).wait_send()


def combine(parts, mix, bias, own, quarter, ep):
    tp, tiles, _, width = parts.shape
    pairs = mix.shape[0]
    tokens = own.shape[0]
    dma = pltpu.SemaphoreType.DMA
    vmem = pl.BlockSpec(memory_space=pltpu.VMEM)
    return pl.pallas_call(
        functools.partial(combine_kernel, ep, tp),
        out_shape=jax.ShapeDtypeStruct((tokens, quarter), BF16),
        in_specs=[vmem] * 4,
        out_specs=vmem,
        scratch_shapes=[
            pltpu.VMEM((tiles, 16, width), BF16),
            pltpu.VMEM((tiles, 16, width), BF16),
            pltpu.VMEM((tiles, 16, width), BF16),
            pltpu.VMEM((tiles, 16, width), BF16),
            pltpu.VMEM((pairs, 32, width), BF16),
            pltpu.VMEM((pairs, 16, width), BF16),
            pltpu.VMEM((pairs, 2, tokens, width), BF16),
            pltpu.VMEM((pairs, 2, tokens, width), BF16),
            pltpu.VMEM((tokens, width), F32),
            dma((pairs, 2, CHUNKS)),
            dma((pairs, 2, CHUNKS)),
            dma((pairs,)),
            dma((pairs,)),
            dma((tiles, 3)),
            dma((tiles, 3)),
        ],
        compiler_params=pltpu.CompilerParams(
            collective_id=1, has_side_effects=True, vmem_limit_bytes=40 << 20
        ),
        name="combine",
    )(parts, mix, bias, own)


def rms_normed(hidden, norm_gain):
    widened = hidden.astype(F32)
    mean_square = jnp.mean(widened * widened, axis=-1, keepdims=True)
    scaled = widened * lax.rsqrt(mean_square + 1e-05) * norm_gain.astype(F32)
    return scaled.astype(BF16)


def shards(
    hidden,
    route_experts,
    route_weight,
    norm_gain,
    gate_up_codes,
    gate_up_scales,
    gate_up_bias,
    down_codes,
    down_scales,
    down_bias,
):
    ep = lax.axis_size("ep")
    tp = lax.axis_size("tp")
    col = lax.axis_index("tp")
    tokens, model_width = hidden.shape
    top = route_experts.shape[1]
    quarter = model_width // tp
    width = -(-(quarter + 2 * top) // 128) * 128
    spare = width - quarter
    normed = rms_normed(hidden, norm_gain)
    own_normed = lax.dynamic_slice_in_dim(normed, col * quarter, quarter, 1)
    block = jnp.concatenate(
        [
            own_normed,
            route_experts.astype(BF16),
            route_weight.astype(BF16),
            jnp.zeros((tokens, spare - 2 * top), BF16),
        ],
        axis=1,
    )
    rows, mix = dispatch(block, ep, tp, top, quarter - (width - 128))
    tiles = rows.shape[1]

    codes = gate_up_codes[0]
    columns = codes.shape[1]
    scales = gate_up_scales[0].astype(F32).reshape(-1, 2, columns)
    hidden_units = down_codes.shape[1]
    words = quarter // 8
    low_codes = jnp.pad(down_codes[0].reshape(hidden_units, tp, words), ((0, 0), (0, 0), (0, 128 - words)))
    low_codes = low_codes.reshape(hidden_units, tp * 128)
    low_scales = jnp.moveaxis(down_scales[0].astype(F32).reshape(-1, tp, quarter), 1, 0)
    low_scales = jnp.pad(low_scales, ((0, 0), (0, 0), (0, spare)))
    parts = experts(
        rows.reshape(tp, tiles * 16, width), codes, scales, gate_up_bias.astype(F32), low_codes, low_scales
    )

    bias = jnp.pad(down_bias.astype(F32), ((0, 0), (0, spare)))
    own = lax.dynamic_slice_in_dim(hidden, col * quarter, quarter, 1)
    own = jnp.pad(own, ((0, 0), (0, spare)))
    return combine(parts.reshape(tp, tiles, 16, width), mix, bias, own, quarter, ep)


def solution(mesh):
    placed = (
        P(("groups", "ep"), None),
        P(("groups", "ep"), None),
        P(("groups", "ep"), None),
        P(),
        P("ep", None, "tp"),
        P("ep", None, "tp"),
        P("ep", "tp"),
        P("ep", "tp", None),
        P("ep", "tp", None),
        P("ep", "tp"),
    )
    return jax.shard_map(
        shards, mesh=mesh, in_specs=placed, out_specs=P(("groups", "ep"), "tp"), check_vma=False
    )
```

```python
import functools

import jax
import jax.numpy as jnp
from jax import lax
from jax.experimental import pallas as pl
from jax.experimental.pallas import tpu as pltpu
from jax.sharding import PartitionSpec as P

CAP = 8
CHUNKS = 2
F32 = jnp.float32
BF16 = jnp.bfloat16


def dot(a, b):
    return jnp.dot(a, b, preferred_element_type=F32)


def iota(shape, dim):
    return lax.broadcasted_iota(jnp.int32, shape, dim)


def neighbours(ep, tp):
    me = lax.axis_index("ep")
    core = lax.rem(me, 2)
    col = lax.axis_index("tp")
    return dict(
        me=me,
        up=lax.rem(me + 2, ep),
        down=lax.rem(me + ep - 2, ep),
        pal=me + 1 - 2 * core,
        core=core,
        col=col,
        right=lax.rem(col + 1, tp),
        left=lax.rem(col + tp - 1, tp),
        across=lax.rem(col + 2, tp),
    )


def greet(at):
    barrier = pltpu.get_barrier_semaphore()
    for place in ({"ep": at["up"]}, {"ep": at["down"]}, {"ep": at["pal"]}, {"tp": at["right"]}, {"tp": at["left"]}):
        pl.semaphore_signal(barrier, inc=1, device_id=place, device_id_type=pl.DeviceIdType.MESH)
    pl.semaphore_wait(barrier, 5)


def remote(src, dst, send, recv, place):
    return pltpu.make_async_remote_copy(
        src_ref=src, dst_ref=dst, send_sem=send, recv_sem=recv, device_id=place, device_id_type=pl.DeviceIdType.MESH
    )


def nibble_value(word, shift):
    top_bits = lax.shift_left(word, 28 - shift)
    magnit = lax.shift_right_logical(top_bits, 28) & 7
    doubled = magnit + jnp.maximum(magnit - 4, 0) + 2 * jnp.maximum(magnit - 6, 0)
    value = doubled.astype(F32)
    return jnp.where(top_bits < 0, -value, value)


def layer_kernel(
    ep, tp, top, meta_at,
    block_ref, codes_hbm, scales_hbm, up_bias_ref, low_codes_hbm, low_scales_ref, down_bias_ref, own_ref,
    out_ref,
    held, handed, rows, mix,
    codes, scales, scales32, low_codes, upper, lower, spread, act, parts,
    across, summed, staged, direct, outs, given, moving, terms, own_sum,
    local_sem, zs, zr, ds, dr, xs, xr, bs, br, zs2, zr2, ds2, dr2, xs2, xr2, ts, tr, fs, fr,
):
    pairs = held.shape[0]
    tokens = held.shape[3]
    width = held.shape[4]
    part = tokens // CHUNKS
    half = pairs // 2
    columns = codes.shape[1]
    hidden_units = lower.shape[1]
    units = upper.shape[0] // tp
    word_rows = codes.shape[0]
    real_units = word_rows // 2 // tp
    words = real_units * 2
    at = neighbours(ep, tp)

    carrier = at["core"] == 1
    fetches = [
        pltpu.make_async_copy(codes_hbm, codes, local_sem.at[1]),
        pltpu.make_async_copy(scales_hbm, scales, local_sem.at[2]),
        pltpu.make_async_copy(low_codes_hbm, low_codes, local_sem.at[3]),
    ]
    for fetch in fetches:
        fetch.start()
    greet(at)

    def piece(pair, b, side, h):
        return held.at[pair, b, side, pl.ds(h * part, part)]

    def hop(s, b, side, h):
        src = piece(s - 1, b, side, h)
        if isinstance(s, int) and s == 1:
            src = piece(0, 0, 0, h) if b == 0 else block_ref.at[pl.ds(h * part, part)]
        place = {"ep": at["up"] if side == 0 else at["down"]}
        return remote(src, piece(s, b, side, h), zs.at[s, b, side, h], zr.at[s, b, side, h], place)

    def last_hop(b, side, h):
        place = {"ep": at["up"] if side == 0 else at["down"]}
        return remote(
            piece(pairs - 1, b, side, h), piece(0, b, 1, h), zs.at[0, b, side, h], zr.at[0, b, side, h], place
        )

    def last_side(h):
        return 0 if h < CHUNKS // 2 else 1

    def hand_block(pair, side):
        return remote(
            held.at[pair, 0, side], held.at[pair, 0, side], bs.at[pair, side], br.at[pair, side],
            {"ep": at["pal"]},
        )

    def lend_block():
        return remote(block_ref, held.at[0, 0, 0], bs.at[0, 0], br.at[0, 0], {"ep": at["pal"]})

    def tile(col, pos, p):
        return rows.at[col, pos * 2 + p]

    def to_pal(pos):
        return remote(handed.at[pos], tile(at["col"], pos, 1), ds.at[pos], dr.at[pos], {"ep": at["pal"]})

    def x_copy(col, pos, p, kind, place):
        return remote(
            tile(col, pos, p), tile(col, pos, p), xs.at[pos * 2 + p, kind], xr.at[pos * 2 + p, kind],
            {"tp": place},
        )

    def go_right(pos, p):
        return x_copy(at["col"], pos, p, 0, at["right"])

    def go_left(pos, p):
        return x_copy(at["col"], pos, p, 1, at["left"])

    def from_left(pos, p):
        return x_copy(at["left"], pos, p, 0, at["right"])

    def from_right(pos, p):
        return x_copy(at["right"], pos, p, 1, at["left"])

    def relay(pos, p):
        if p == 0:
            return x_copy(at["left"], pos, p, 2, at["right"])
        return x_copy(at["right"], pos, p, 2, at["left"])

    def relayed(pos, p):
        return x_copy(at["across"], pos, p, 2, at["right"])

    @pl.when(jnp.logical_not(carrier))
    def _():
        lend_block().start()

    @pl.when(carrier)
    def _():
        for h in range(CHUNKS):
            for side in range(2):
                hop(1, 1, side, h).start()
        lend_block().wait_recv()
        for h in range(CHUNKS):
            for side in range(2):
                hop(1, 0, side, h).start()
        held[0, 1, 0] = block_ref[...]

    @pl.when(jnp.logical_not(carrier))
    def _():
        held[0, 0, 0] = block_ref[...]

    both = 2 * tokens
    lane = iota((both, 128), 1)
    ls = iota((128, 128), 1)
    own_cols = (ls < 16).astype(BF16)
    pal_cols = ((ls >= 16) & (ls < 32)).astype(BF16)
    ti, tj = iota((both, both), 0), iota((both, both), 1)
    earlier = ((tj < ti) & ((ti < tokens) == (tj < tokens))).astype(BF16)
    wanted = (lax.rem(lane, 16) - jnp.where(iota((both, 128), 0) >= tokens, 8, 0)).astype(F32)
    id_lanes = (lane >= meta_at) & (lane < meta_at + top)
    own_id = at["me"].astype(F32)
    pal_id = at["pal"].astype(F32)

    def select(pair, pos):
        block = held[pair, at["core"]].reshape(both, width)
        meta = block[:, width - 128 :].astype(F32)
        weights = pltpu.roll(meta, 128 - top, axis=1)
        is_own = id_lanes & (meta == own_id)
        is_pal = id_lanes & (meta == pal_id)
        match = dot(jnp.where(is_own, 1.0, 0.0).astype(BF16), own_cols) + dot(
            jnp.where(is_pal, 1.0, 0.0).astype(BF16), pal_cols
        )
        weight = dot(jnp.where(is_own, weights, 0.0).astype(BF16), own_cols) + dot(
            jnp.where(is_pal, weights, 0.0).astype(BF16), pal_cols
        )
        slot = dot(earlier, match.astype(BF16))
        placed = (match > 0.5) & (slot == wanted)
        mix[pair] = jnp.where(placed, weight, 0.0).astype(BF16)
        pick = jnp.transpose(jnp.where(placed, 1.0, 0.0))[:32].astype(BF16)
        picked = dot(pick, block).astype(BF16)
        rows[at["col"], pos * 2] = picked[:16]
        handed[pos] = picked[16:]

    for q in range(tp):
        upper[q * units + real_units : (q + 1) * units] = jnp.zeros((units - real_units, 16, columns), BF16)
    word, lanes = iota((128, width), 0), iota((128, width), 1)
    for j in range(8):
        spread[j * 128 : (j + 1) * 128] = (lanes == 8 * word + j).astype(BF16)
    for fetch in fetches:
        fetch.wait()
    scales32[...] = 0.5 * scales[...].astype(F32)

    def decode(u):
        packed = codes[pl.ds(pl.multiple_of(u * 8, 8), 8), :]
        shift = 4 * iota((8, 8, columns), 1)
        value = nibble_value(jnp.broadcast_to(packed[:, None, :], (8, 8, columns)), shift)
        value = value.reshape(2, 32, columns)
        for k in range(2):
            scaled = (value[k] * scales32[pl.ds(2 * u + k, 1), :]).astype(BF16).reshape(2, 16, columns)
            for m in range(2):
                unit = 4 * u + 2 * k + m
                upper[unit + (units - real_units) * (unit // real_units)] = scaled[m]

    low_parts = max(1, pairs // tp)
    low_rows = hidden_units // low_parts
    low_each = tp * low_parts // pairs
    low_lanes = low_codes.shape[1]
    window = min(256, low_lanes)

    def decode_low(i):
        q, r = i // low_parts, lax.rem(i, low_parts)
        begin = jnp.minimum(128 * ((words * q) // 128), low_lanes - window)
        packed = low_codes[
            pl.ds(pl.multiple_of(r * low_rows, 32), low_rows), pl.ds(pl.multiple_of(begin, 128), window)
        ]
        packed = pltpu.roll(packed, lax.rem(window + begin - words * q, window), axis=1)[:, :128]
        whole = jnp.concatenate([nibble_value(packed, 4 * j).astype(BF16) for j in range(8)], axis=1)
        value = dot(whole, spread[...]).reshape(low_rows // 32, 32, width)
        value = value * low_scales_ref[i][:, None, :]
        lower[q, pl.ds(pl.multiple_of(r * low_rows, 32), low_rows)] = value.reshape(low_rows, width).astype(BF16)

    tiles_n = columns // 256
    si, sj = iota((256, 128), 0), iota((256, 128), 1)
    evens = (si == 2 * sj).astype(BF16)

    def project(n, part_at):
        at_n = pl.ds(pl.multiple_of(n * 256, 256), 256)
        total = jnp.broadcast_to(up_bias_ref[:, at_n], (16 * pairs, 256))
        for q in range(tp):
            weight = upper[q * units : (q + 1) * units, :, at_n].reshape(units * 16, 256)
            given_rows = rows[q, part_at * pairs : (part_at + 1) * pairs].reshape(16 * pairs, width)
            total = total + dot(given_rows, weight)
        gate = jnp.minimum(total, 7.0)
        upward = jnp.clip(pltpu.roll(total, 255, axis=1), -7.0, 7.0)
        value = (gate * jax.nn.sigmoid(1.702 * gate) * (upward + 1.0)).astype(BF16)
        act[part_at, :, pl.ds(pl.multiple_of(n * 128, 128), 128)] = dot(value, evens).astype(BF16)

    def project_down(q, part_at):
        value = dot(act[part_at], lower[q]).astype(BF16)
        parts[q, part_at * pairs : (part_at + 1) * pairs] = value.reshape(pairs, 16, width)

    lag = 2
    project_from = half + 2 * lag + 1
    projected = max(0, min(tiles_n, pairs + 2 * lag - project_from))
    decodes = word_rows // 8
    per_step = -(-decodes // min(pairs - 1, project_from))
    decode_steps = -(-decodes // per_step)

    def arrive(pos, carry):
        from_right(pos, 0).wait_recv()
        from_left(pos, 1).wait_recv()
        for p in range(2):
            relayed(pos, p).wait_recv()
        return carry

    def gather(u, carry):
        @pl.when(carrier & (u < pairs - 1))
        def _():
            s = u + 1
            for h in range(CHUNKS):
                for b in (1, 0):
                    for side in range(2):
                        hop(s, b, side, h).wait_recv()

                        @pl.when(s < pairs - 1)
                        def _():
                            hop(s + 1, b, side, h).start()

                        if side == last_side(h):

                            @pl.when(s == pairs - 1)
                            def _():
                                last_hop(b, side, h).start()

                        if b == 0 and h == CHUNKS - 1:
                            hand_block(s, side).start()

        @pl.when(carrier & (u == pairs - 1))
        def _():
            for b in range(2):
                for h in range(CHUNKS):
                    last_hop(b, last_side(h), h).wait_recv()
            hand_block(0, 1).start()

        @pl.when(u < decode_steps)
        def _():
            for k in range(per_step):
                if per_step * decode_steps == decodes:
                    decode(u * per_step + k)
                else:

                    @pl.when(u * per_step + k < decodes)
                    def _():
                        decode(u * per_step + k)

        @pl.when(jnp.logical_not(carrier) & (u < pairs - 1))
        def _():
            for side in range(2):
                hand_block(u + 1, side).wait_recv()

        @pl.when(jnp.logical_not(carrier) & (u == pairs - 1))
        def _():
            hand_block(0, 1).wait_recv()

        @pl.when(u < pairs)
        def _():
            select(lax.rem(u + 1, pairs), u)
            to_pal(u).start()
            go_right(u, 0).start()
            go_left(u, 0).start()

        @pl.when((u >= lag) & (u < pairs + lag))
        def _():
            to_pal(u - lag).wait_recv()
            go_right(u - lag, 1).start()
            go_left(u - lag, 1).start()
            from_left(u - lag, 0).wait_recv()
            relay(u - lag, 0).start()

        @pl.when(u >= 2 * lag)
        def _():
            from_right(u - 2 * lag, 1).wait_recv()
            relay(u - 2 * lag, 1).start()

        @pl.when(u < pairs)
        def _():
            for k in range(low_each):
                decode_low(u * low_each + k)

        if projected:

            @pl.when(u == project_from)
            def _():
                lax.fori_loop(0, half, arrive, 0)

            @pl.when((u >= project_from) & (u < project_from + projected))
            def _():
                project(u - project_from, 0)

        return carry

    lax.fori_loop(0, pairs + 2 * lag, gather, 0)
    lax.fori_loop(half if projected else 0, pairs, arrive, 0)

    def project_rest(n, carry):
        project(n, 0)
        return carry

    def project_late(n, carry):
        project(n, 1)
        return carry

    def down_late(q, carry):
        project_down(q, 1)
        return carry

    if projected < tiles_n:
        lax.fori_loop(projected, tiles_n, project_rest, 0)
    lax.fori_loop(0, tiles_n, project_late, 0)
    lax.fori_loop(0, tp, down_late, 0)

    def out_side(h):
        return 1 if h < CHUNKS // 2 else 0

    def up_or_down(side):
        return {"ep": at["up"] if side == 1 else at["down"]}

    def sum_hop(s, b, side, h):
        src = moving.at[s, b, side, pl.ds(h * part, part)]
        dst = moving.at[s - 1, b, side, pl.ds(h * part, part)]
        return remote(src, dst, zs2.at[s - 1, b, side, h], zr2.at[s - 1, b, side, h], up_or_down(side))

    def first_sum(b, side, h):
        src = terms.at[0, b, 1, pl.ds(h * part, part)]
        dst = moving.at[pairs - 1, b, side, pl.ds(h * part, part)]
        return remote(
            src, dst, zs2.at[pairs - 1, b, side, h], zr2.at[pairs - 1, b, side, h], up_or_down(side)
        )

    def lend_terms(pair):
        return remote(terms.at[pair, 0], terms.at[pair, 0], ts.at[pair], tr.at[pair], {"ep": at["pal"]})

    def hand_sum(side):
        return remote(moving.at[0, 0, side], moving.at[0, 0, side], fs.at[side], fr.at[side], {"ep": at["pal"]})

    def far(p):
        return {"tp": at["right"] if p == 0 else at["left"]}

    def near(p):
        return {"tp": at["left"] if p == 0 else at["right"]}

    def two_away(t, p):
        return remote(parts.at[at["across"], t], across.at[t], xs2.at[t, 0], xr2.at[t, 0], far(p))

    def one_away(t, p):
        col = at["left"] if p == 0 else at["right"]
        return remote(parts.at[col, t], direct.at[t], xs2.at[t, 1], xr2.at[t, 1], near(p))

    def onward(t, p):
        return remote(staged.at[t], summed.at[t], xs2.at[t, 2], xr2.at[t, 2], far(p))

    def give(pos):
        return remote(given.at[pos], outs.at[pos, pl.ds(16, 16)], ds2.at[pos], dr2.at[pos], {"ep": at["pal"]})

    for h in range(CHUNKS):
        side = 1 - out_side(h)
        for b in range(2):
            moving[pairs - 1, b, side, h * part : (h + 1) * part] = jnp.zeros((part, width), BF16)

    down_each = -(-tp // (half - 1)) if half > 1 else tp

    if half <= 1:
        for q in range(tp):
            project_down(q, 0)

    def scatter(t, carry):
        @pl.when(t < pairs)
        def _():
            pos = pairs - 1 - t
            for p in range(2):
                two_away(pos * 2 + p, p).start()
            for p in range(2):
                one_away(pos * 2 + p, p).start()

        @pl.when(carrier & (t >= 8))
        def _():
            u = t - 8
            pair = lax.rem(pairs - u, pairs)
            lend_terms(pair).wait_recv()

            @pl.when(u == 0)
            def _():
                for h in range(CHUNKS):
                    for b in range(2):
                        first_sum(b, out_side(h), h).start()

            @pl.when(u > 0)
            def _():
                for h in range(CHUNKS):
                    for b in (1, 0):
                        for side in (out_side(h), 1 - out_side(h)):
                            rows_at = pl.ds(h * part, part)
                            arrival = remote(
                                moving.at[pair, b, side, rows_at],
                                moving.at[pair, b, side, rows_at],
                                zs2.at[pair, b, side, h],
                                zr2.at[pair, b, side, h],
                                up_or_down(side),
                            )
                            if side == out_side(h):
                                arrival.wait_recv()
                            else:

                                @pl.when(u > 1)
                                def _():
                                    arrival.wait_recv()

                            value = moving[pair, b, side, rows_at].astype(F32) + terms[
                                pair, b, side, rows_at
                            ].astype(F32)
                            moving[pair, b, side, rows_at] = value.astype(BF16)
                            sum_hop(pair, b, side, h).start()

        @pl.when((t >= 6) & (t < pairs + 6))
        def _():
            pos = pairs + 5 - t
            pair = lax.rem(pos + 1, pairs)
            give(pos).wait_recv()
            mixed = dot(mix[pair][:, :32], outs[pos])
            terms[pair, at["core"]] = mixed.astype(BF16).reshape(2, tokens, width)

            @pl.when(t == 6)
            def _():
                own_sum[...] = mixed[:tokens]

            @pl.when(jnp.logical_not(carrier))
            def _():
                lend_terms(pair).start()

        @pl.when((t >= 2) & (t < pairs + 2))
        def _():
            for p in range(2):
                t1 = (pairs + 1 - t) * 2 + p
                two_away(t1, p).wait_recv()
                col = at["right"] if p == 0 else at["left"]
                staged[t1] = (across[t1].astype(F32) + parts[col, t1].astype(F32)).astype(BF16)
                onward(t1, p).start()

        @pl.when((t >= 4) & (t < pairs + 4))
        def _():
            pos = pairs + 3 - t
            for p in (1, 0):
                t2 = pos * 2 + p
                one_away(t2, p).wait_recv()
                onward(t2, p).wait_recv()
                total = (
                    summed[t2].astype(F32)
                    + direct[t2].astype(F32)
                    + parts[at["col"], t2].astype(F32)
                    + down_bias_ref[...]
                ).astype(BF16)
                if p == 1:
                    given[pos] = total
                    give(pos).start()
                else:
                    outs[pos, :16] = total

        if half > 1:
            for k in range(down_each):
                q = (t - 1) * down_each + k

                @pl.when((t >= 1) & (q < tp))
                def _():
                    project_down(q, 0)

        return carry

    lax.fori_loop(0, pairs + 8, scatter, 0)

    @pl.when(carrier)
    def _():
        for b in range(2):
            for side in range(2):
                for h in range(CHUNKS):
                    sum_hop(1, b, side, h).wait_recv()
                if b == 0:
                    hand_sum(side).start()

    @pl.when(jnp.logical_not(carrier))
    def _():
        for side in range(2):
            hand_sum(side).wait_recv()

    core = at["core"]
    total = own_ref[...].astype(F32) + own_sum[...]
    total = total + moving[0, core, 0].astype(F32) + moving[0, core, 1].astype(F32)
    out_ref[...] = total[:, : out_ref.shape[1]].astype(BF16)

    def finish(pos, carry):
        to_pal(pos).wait_send()
        give(pos).wait_send()
        for p in range(2):
            go_right(pos, p).wait_send()
            go_left(pos, p).wait_send()
            relay(pos, p).wait_send()
            two_away(pos * 2 + p, p).wait_send()
            one_away(pos * 2 + p, p).wait_send()
            onward(pos * 2 + p, p).wait_send()
        return carry

    lax.fori_loop(0, pairs, finish, 0)

    @pl.when(carrier)
    def _():
        def sent(s, carry):
            for b in range(2):
                for side in range(2):
                    for h in range(CHUNKS):
                        hop(s, b, side, h).wait_send()
                        sum_hop(s, b, side, h).wait_send()
            for side in range(2):
                hand_block(s, side).wait_send()
            return carry

        lax.fori_loop(1, pairs, sent, 0)
        hand_block(0, 1).wait_send()
        for b in range(2):
            for h in range(CHUNKS):
                last_hop(b, last_side(h), h).wait_send()
                first_sum(b, out_side(h), h).wait_send()
        for side in range(2):
            hand_sum(side).wait_send()

    @pl.when(jnp.logical_not(carrier))
    def _():
        lend_block().wait_send()

        def lent(pair, carry):
            lend_terms(pair).wait_send()
            return carry

        lax.fori_loop(0, pairs, lent, 0)


def layer(block, codes, scales, up_bias, low_codes, low_scales, down_bias, own, quarter, ep, tp, top):
    tokens, width = block.shape
    pairs = ep // 4
    word_rows, columns = codes.shape
    hidden_units, low_lanes = low_codes.shape
    tiles = 2 * pairs
    dma = pltpu.SemaphoreType.DMA
    vmem = pl.BlockSpec(memory_space=pltpu.VMEM)
    hbm = pl.BlockSpec(memory_space=pl.ANY)
    ring = dma((pairs, 2, 2, CHUNKS))
    return pl.pallas_call(
        functools.partial(layer_kernel, ep, tp, top, quarter - (width - 128)),
        out_shape=jax.ShapeDtypeStruct((tokens, quarter), BF16),
        in_specs=[vmem, hbm, hbm, vmem, hbm, vmem, vmem, vmem],
        out_specs=vmem,
        scratch_shapes=[
            pltpu.VMEM((pairs, 2, 2, tokens, width), BF16),
            pltpu.VMEM((pairs, 16, width), BF16),
            pltpu.VMEM((tp, tiles, 16, width), BF16),
            pltpu.VMEM((pairs, 2 * tokens, 128), BF16),
            pltpu.VMEM((word_rows, columns), jnp.int32),
            pltpu.VMEM(scales.shape, BF16),
            pltpu.VMEM(scales.shape, F32),
            pltpu.VMEM((hidden_units, low_lanes), jnp.int32),
            pltpu.VMEM((tp * width // 16, 16, columns), BF16),
            pltpu.VMEM((tp, hidden_units, width), BF16),
            pltpu.VMEM((1024, width), BF16),
            pltpu.VMEM((2, 16 * pairs, hidden_units), BF16),
            pltpu.VMEM((tp, tiles, 16, width), BF16),
            pltpu.VMEM((tiles, 16, width), BF16),
            pltpu.VMEM((tiles, 16, width), BF16),
            pltpu.VMEM((tiles, 16, width), BF16),
            pltpu.VMEM((tiles, 16, width), BF16),
            pltpu.VMEM((pairs, 32, width), BF16),
            pltpu.VMEM((pairs, 16, width), BF16),
            pltpu.VMEM((pairs, 2, 2, tokens, width), BF16),
            pltpu.VMEM((pairs, 2, 2, tokens, width), BF16),
            pltpu.VMEM((tokens, width), F32),
            dma((4,)),
            ring, ring, dma((pairs,)), dma((pairs,)), dma((tiles, 3)), dma((tiles, 3)),
            dma((pairs, 2)), dma((pairs, 2)),
            ring, ring, dma((pairs,)), dma((pairs,)), dma((tiles, 3)), dma((tiles, 3)),
            dma((pairs,)), dma((pairs,)), dma((2,)), dma((2,)),
        ],
        compiler_params=pltpu.CompilerParams(
            collective_id=0, has_side_effects=True, vmem_limit_bytes=60 << 20
        ),
        name="layer",
    )(block, codes, scales, up_bias, low_codes, low_scales, down_bias, own)


def rms_normed(hidden, norm_gain):
    widened = hidden.astype(F32)
    mean_square = jnp.mean(widened * widened, axis=-1, keepdims=True)
    scaled = widened * lax.rsqrt(mean_square + 1e-05) * norm_gain.astype(F32)
    return scaled.astype(BF16)


def shards(
    hidden,
    route_experts,
    route_weight,
    norm_gain,
    gate_up_codes,
    gate_up_scales,
    gate_up_bias,
    down_codes,
    down_scales,
    down_bias,
):
    ep = lax.axis_size("ep")
    tp = lax.axis_size("tp")
    col = lax.axis_index("tp")
    tokens, model_width = hidden.shape
    top = route_experts.shape[1]
    quarter = model_width // tp
    width = -(-(quarter + 2 * top) // 128) * 128
    spare = width - quarter
    normed = rms_normed(hidden, norm_gain)
    own_normed = lax.dynamic_slice_in_dim(normed, col * quarter, quarter, 1)
    block = jnp.concatenate(
        [
            own_normed,
            route_experts.astype(BF16),
            route_weight.astype(BF16),
            jnp.zeros((tokens, spare - 2 * top), BF16),
        ],
        axis=1,
    )
    hidden_units = down_codes.shape[1]
    low_codes = jnp.pad(down_codes[0], ((0, 0), (0, -(down_codes.shape[2]) % 128)))
    low_parts = max(1, ep // 4 // tp)
    low_scales = 0.5 * down_scales[0].astype(F32).reshape(-1, tp, quarter)
    low_scales = jnp.pad(jnp.moveaxis(low_scales, 1, 0), ((0, 0), (0, 0), (0, spare)))
    low_scales = low_scales.reshape(tp * low_parts, hidden_units // 32 // low_parts, width)
    bias = jnp.pad(down_bias.astype(F32), ((0, 0), (0, spare)))
    own = lax.dynamic_slice_in_dim(hidden, col * quarter, quarter, 1)
    own = jnp.pad(own, ((0, 0), (0, spare)))
    return layer(
        block, gate_up_codes[0], gate_up_scales[0], gate_up_bias.astype(F32), low_codes, low_scales, bias, own,
        quarter, ep, tp, top,
    )


def solution(mesh):
    placed = (
        P(("groups", "ep"), None),
        P(("groups", "ep"), None),
        P(("groups", "ep"), None),
        P(),
        P("ep", None, "tp"),
        P("ep", None, "tp"),
        P("ep", "tp"),
        P("ep", "tp", None),
        P("ep", "tp", None),
        P("ep", "tp"),
    )
    return jax.shard_map(
        shards, mesh=mesh, in_specs=placed, out_specs=P(("groups", "ep"), "tp"), check_vma=False
    )
```

```python
import functools

import jax
import jax.numpy as jnp
from jax import lax
from jax.experimental import pallas as pl
from jax.experimental.pallas import tpu as pltpu
from jax.sharding import PartitionSpec as P

CAP = 8
CHUNKS = 4
F32 = jnp.float32
BF16 = jnp.bfloat16


def dot(a, b):
    return jnp.dot(a, b, preferred_element_type=F32)


def iota(shape, dim):
    return lax.broadcasted_iota(jnp.int32, shape, dim)


def neighbours(ep, tp):
    me = lax.axis_index("ep")
    core = lax.rem(me, 2)
    col = lax.axis_index("tp")
    return dict(
        me=me,
        up=lax.rem(me + 3 - 2 * core, ep),
        down=lax.rem(me + ep - 1 - 2 * core, ep),
        pal=me + 1 - 2 * core,
        col=col,
        right=lax.rem(col + 1, tp),
        left=lax.rem(col + tp - 1, tp),
        across=lax.rem(col + 2, tp),
    )


def greet(at):
    barrier = pltpu.get_barrier_semaphore()
    for place in ({"ep": at["up"]}, {"ep": at["down"]}, {"ep": at["pal"]}, {"tp": at["right"]}, {"tp": at["left"]}):
        pl.semaphore_signal(barrier, inc=1, device_id=place, device_id_type=pl.DeviceIdType.MESH)
    pl.semaphore_wait(barrier, 5)


def remote(src, dst, send, recv, place):
    return pltpu.make_async_remote_copy(
        src_ref=src, dst_ref=dst, send_sem=send, recv_sem=recv, device_id=place, device_id_type=pl.DeviceIdType.MESH
    )


def nibble_value(word, shift):
    top_bits = lax.shift_left(word, 28 - shift)
    magnit = lax.shift_right_logical(top_bits, 28) & 7
    doubled = magnit + jnp.maximum(magnit - 4, 0) + 2 * jnp.maximum(magnit - 6, 0)
    value = doubled.astype(F32)
    return jnp.where(top_bits < 0, -value, value)


def layer_kernel(
    ep, tp, top, meta_at,
    hidden_ref, ids_ref, weights_ref, gain_ref, codes_hbm, scales_hbm, up_bias_ref, low_codes_hbm,
    low_scales_hbm, down_bias_ref,
    out_ref,
    turned_codes,    wide, wide_scales, narrow_scales, low_scales, down_bias, own, block_ref, held, handed, rows, mix,
    codes, scales, scales32, low_codes, upper, lower, spread, act, parts,
    across, summed, staged, direct, outs, given, moving, terms, own_sum,
    local_sem, zs, zr, ds, dr, xs, xr, zs2, zr2, ds2, dr2, xs2, xr2,
):
    pairs = held.shape[0]
    tokens = held.shape[2]
    width = held.shape[3]
    part = tokens // CHUNKS
    half = pairs // 2
    columns = codes.shape[1]
    hidden_units = lower.shape[1]
    units = upper.shape[0] // tp
    word_rows = codes.shape[0]
    real_units = word_rows // 2 // tp
    words = real_units * 2
    at = neighbours(ep, tp)

    fetches = [
        pltpu.make_async_copy(codes_hbm, codes, local_sem.at[1]),
        pltpu.make_async_copy(scales_hbm, scales, local_sem.at[2]),
        pltpu.make_async_copy(low_codes_hbm, turned_codes.at[pl.ds(0, low_codes_hbm.shape[0])], local_sem.at[3]),
        pltpu.make_async_copy(low_scales_hbm, narrow_scales, local_sem.at[0]),
    ]
    for fetch in fetches:
        fetch.start()

    model_width = hidden_ref.shape[1]
    quarter = out_ref.shape[1]
    whole_width = wide.shape[1]
    rest = jnp.zeros((tokens, whole_width - model_width), F32)
    widened = hidden_ref[...].astype(F32)
    mean_square = jnp.mean(widened * widened, axis=-1, keepdims=True)
    back = lax.rem(whole_width - at["col"] * quarter, whole_width)
    wide[:, :model_width] = widened
    wide[:, model_width:] = rest
    own[...] = pltpu.roll(wide[...], back, axis=1)[:, :width]
    wide[:8, :model_width] = jnp.broadcast_to(gain_ref[...].astype(F32), (8, model_width))
    gain = pltpu.roll(wide[:8], back, axis=1)[:1, :width]
    normed = (own[...] * lax.rsqrt(mean_square + 1e-05) * gain).astype(BF16).astype(F32)
    choice, meta_lane = iota((top, 128), 0), iota((top, 128), 1)
    meta_own = dot(ids_ref[...].astype(F32).astype(BF16), (meta_lane == meta_at + choice).astype(BF16))
    meta_own = meta_own + dot(
        weights_ref[...].astype(BF16), (meta_lane == meta_at + top + choice).astype(BF16)
    )
    if width > 128:
        block_ref[:, : width - 128] = normed[:, : width - 128].astype(BF16)
    is_data = iota((tokens, 128), 1) < meta_at
    block_ref[:, width - 128 :] = jnp.where(is_data, normed[:, width - 128 :], meta_own).astype(BF16)
    greet(at)

    def piece(pair, side, h):
        return held.at[pair, side, pl.ds(h * part, part)]

    def hop(s, side, h):
        src = piece(s - 1, side, h)
        if isinstance(s, int) and s == 1:
            src = block_ref.at[pl.ds(h * part, part)]
        place = {"ep": at["up"] if side == 0 else at["down"]}
        return remote(src, piece(s, side, h), zs.at[s, side, h], zr.at[s, side, h], place)

    def last_hop(side, h):
        place = {"ep": at["up"] if side == 0 else at["down"]}
        return remote(
            piece(pairs - 1, side, h), piece(0, 1, h), zs.at[0, side, h], zr.at[0, side, h], place
        )

    def last_side(h):
        return 0 if h < CHUNKS // 2 else 1

    def tile(col, pos, p):
        return rows.at[col, pos * 2 + p]

    def to_pal(pos):
        return remote(handed.at[pos], tile(at["col"], pos, 1), ds.at[pos], dr.at[pos], {"ep": at["pal"]})

    def x_copy(col, pos, p, kind, place):
        return remote(
            tile(col, pos, p), tile(col, pos, p), xs.at[pos * 2 + p, kind], xr.at[pos * 2 + p, kind],
            {"tp": place},
        )

    def go_right(pos, p):
        return x_copy(at["col"], pos, p, 0, at["right"])

    def go_left(pos, p):
        return x_copy(at["col"], pos, p, 1, at["left"])

    def from_left(pos, p):
        return x_copy(at["left"], pos, p, 0, at["right"])

    def from_right(pos, p):
        return x_copy(at["right"], pos, p, 1, at["left"])

    def relay(pos, p):
        if p == 0:
            return x_copy(at["left"], pos, p, 2, at["right"])
        return x_copy(at["right"], pos, p, 2, at["left"])

    def relayed(pos, p):
        return x_copy(at["across"], pos, p, 2, at["right"])

    for h in range(CHUNKS):
        for side in range(2):
            hop(1, side, h).start()
    held[0, 0] = block_ref[...]

    both = 2 * tokens
    lane = iota((both, 128), 1)
    ls = iota((128, 128), 1)
    own_cols = (ls < 16).astype(BF16)
    pal_cols = ((ls >= 16) & (ls < 32)).astype(BF16)
    ti, tj = iota((both, both), 0), iota((both, both), 1)
    earlier = ((tj < ti) & ((ti < tokens) == (tj < tokens))).astype(BF16)
    wanted = (lax.rem(lane, 16) - jnp.where(iota((both, 128), 0) >= tokens, 8, 0)).astype(F32)
    id_lanes = (lane >= meta_at) & (lane < meta_at + top)
    own_id = at["me"].astype(F32)
    pal_id = at["pal"].astype(F32)

    def select(pair, pos):
        block = held[pair].reshape(both, width)
        meta = block[:, width - 128 :].astype(F32)
        weights = pltpu.roll(meta, 128 - top, axis=1)
        is_own = id_lanes & (meta == own_id)
        is_pal = id_lanes & (meta == pal_id)
        match = dot(jnp.where(is_own, 1.0, 0.0).astype(BF16), own_cols) + dot(
            jnp.where(is_pal, 1.0, 0.0).astype(BF16), pal_cols
        )
        weight = dot(jnp.where(is_own, weights, 0.0).astype(BF16), own_cols) + dot(
            jnp.where(is_pal, weights, 0.0).astype(BF16), pal_cols
        )
        slot = dot(earlier, match.astype(BF16))
        placed = (match > 0.5) & (slot == wanted)
        mix[pair] = jnp.where(placed, weight, 0.0).astype(BF16)
        pick = jnp.transpose(jnp.where(placed, 1.0, 0.0))[:32].astype(BF16)
        picked = dot(pick, block).astype(BF16)
        rows[at["col"], pos * 2] = picked[:16]
        handed[pos] = picked[16:]

    for q in range(tp):
        upper[q * units + real_units : (q + 1) * units] = jnp.zeros((units - real_units, 16, columns), BF16)
    word, lanes = iota((128, width), 0), iota((128, width), 1)
    for j in range(8):
        spread[j * 128 : (j + 1) * 128] = (lanes == 8 * word + j).astype(BF16)
    for fetch in fetches:
        fetch.wait()
    turned_codes[words * tp :] = jnp.zeros((turned_codes.shape[0] - words * tp, hidden_units), jnp.int32)
    low_codes[...] = jnp.transpose(turned_codes[...])
    scales32[...] = 0.5 * scales[...].astype(F32)
    low_parts = max(1, pairs // tp)
    blocks = wide_scales.shape[0]
    each = blocks // low_parts
    wide_scales[:, :model_width] = 0.5 * narrow_scales[...].astype(F32)
    wide_scales[:, model_width:] = jnp.zeros((blocks, whole_width - model_width), F32)
    for q in range(tp):
        turned = wide_scales[...]
        if q:
            turned = pltpu.roll(turned, whole_width - q * quarter, axis=1)
        turned = jnp.where(iota((blocks, width), 1) < quarter, turned[:, :width], 0.0)
        for r in range(low_parts):
            low_scales[q * low_parts + r] = turned[r * each : (r + 1) * each]
    down_bias[...] = jnp.zeros_like(down_bias)
    down_bias[:, :quarter] = down_bias_ref[...].astype(F32)

    def decode(u):
        packed = codes[pl.ds(pl.multiple_of(u * 8, 8), 8), :]
        shift = 4 * iota((8, 8, columns), 1)
        value = nibble_value(jnp.broadcast_to(packed[:, None, :], (8, 8, columns)), shift)
        value = value.reshape(2, 32, columns)
        for k in range(2):
            scaled = (value[k] * scales32[pl.ds(2 * u + k, 1), :]).astype(BF16).reshape(2, 16, columns)
            for m in range(2):
                unit = 4 * u + 2 * k + m
                upper[unit + (units - real_units) * (unit // real_units)] = scaled[m]

    low_rows = hidden_units // low_parts
    low_each = tp * low_parts // pairs
    low_lanes = low_codes.shape[1]
    window = min(256, low_lanes)

    def decode_low(i):
        q, r = i // low_parts, lax.rem(i, low_parts)
        begin = jnp.minimum(128 * ((words * q) // 128), low_lanes - window)
        packed = low_codes[
            pl.ds(pl.multiple_of(r * low_rows, 32), low_rows), pl.ds(pl.multiple_of(begin, 128), window)
        ]
        packed = pltpu.roll(packed, lax.rem(window + begin - words * q, window), axis=1)[:, :128]
        whole = jnp.concatenate([nibble_value(packed, 4 * j).astype(BF16) for j in range(8)], axis=1)
        value = dot(whole, spread[...]).reshape(low_rows // 32, 32, width)
        value = value * low_scales[i][:, None, :]
        lower[q, pl.ds(pl.multiple_of(r * low_rows, 32), low_rows)] = value.reshape(low_rows, width).astype(BF16)

    tiles_n = columns // 256
    si, sj = iota((256, 128), 0), iota((256, 128), 1)
    evens = (si == 2 * sj).astype(BF16)

    def project(n, part_at):
        at_n = pl.ds(pl.multiple_of(n * 256, 256), 256)
        total = jnp.broadcast_to(up_bias_ref[:, at_n].astype(F32), (16 * pairs, 256))
        for q in range(tp):
            weight = upper[q * units : (q + 1) * units, :, at_n].reshape(units * 16, 256)
            given_rows = rows[q, part_at * pairs : (part_at + 1) * pairs].reshape(16 * pairs, width)
            total = total + dot(given_rows, weight)
        gate = jnp.minimum(total, 7.0)
        upward = jnp.clip(pltpu.roll(total, 255, axis=1), -7.0, 7.0)
        value = (gate * jax.nn.sigmoid(1.702 * gate) * (upward + 1.0)).astype(BF16)
        act[part_at, :, pl.ds(pl.multiple_of(n * 128, 128), 128)] = dot(value, evens).astype(BF16)

    def project_down(q, part_at):
        value = dot(act[part_at], lower[q]).astype(BF16)
        parts[q, part_at * pairs : (part_at + 1) * pairs] = value.reshape(pairs, 16, width)

    lag = 2
    project_from = half + 2 * lag + 1
    projected = max(0, min(tiles_n, pairs + 2 * lag - project_from))
    decodes = word_rows // 8
    per_step = -(-decodes // min(pairs - 1, project_from))
    decode_steps = -(-decodes // per_step)

    def arrive(pos, carry):
        from_right(pos, 0).wait_recv()
        from_left(pos, 1).wait_recv()
        for p in range(2):
            relayed(pos, p).wait_recv()
        return carry

    def gather(u, carry):
        @pl.when(u < pairs - 1)
        def _():
            s = u + 1
            for h in range(CHUNKS):
                for side in range(2):
                    hop(s, side, h).wait_recv()

                    @pl.when(s < pairs - 1)
                    def _():
                        hop(s + 1, side, h).start()

                    if side == last_side(h):

                        @pl.when(s == pairs - 1)
                        def _():
                            last_hop(side, h).start()

        @pl.when(u == pairs - 1)
        def _():
            for h in range(CHUNKS):
                last_hop(last_side(h), h).wait_recv()

        @pl.when(u < decode_steps)
        def _():
            for k in range(per_step):
                if per_step * decode_steps == decodes:
                    decode(u * per_step + k)
                else:

                    @pl.when(u * per_step + k < decodes)
                    def _():
                        decode(u * per_step + k)

        @pl.when(u < pairs)
        def _():
            select(lax.rem(u + 1, pairs), u)
            to_pal(u).start()
            go_right(u, 0).start()
            go_left(u, 0).start()

        @pl.when((u >= lag) & (u < pairs + lag))
        def _():
            to_pal(u - lag).wait_recv()
            go_right(u - lag, 1).start()
            go_left(u - lag, 1).start()
            from_left(u - lag, 0).wait_recv()
            relay(u - lag, 0).start()

        @pl.when(u >= 2 * lag)
        def _():
            from_right(u - 2 * lag, 1).wait_recv()
            relay(u - 2 * lag, 1).start()

        @pl.when(u < pairs)
        def _():
            for k in range(low_each):
                decode_low(u * low_each + k)

        if projected:

            @pl.when(u == project_from)
            def _():
                lax.fori_loop(0, half, arrive, 0)

            @pl.when((u >= project_from) & (u < project_from + projected))
            def _():
                project(u - project_from, 0)

        return carry

    lax.fori_loop(0, pairs + 2 * lag, gather, 0)
    lax.fori_loop(half if projected else 0, pairs, arrive, 0)

    def project_rest(n, carry):
        project(n, 0)
        return carry

    def project_late(n, carry):
        project(n, 1)
        return carry

    def down_late(q, carry):
        project_down(q, 1)
        return carry

    if projected < tiles_n:
        lax.fori_loop(projected, tiles_n, project_rest, 0)
    lax.fori_loop(0, tiles_n, project_late, 0)
    lax.fori_loop(0, tp, down_late, 0)

    def out_side(h):
        return 1 if h < CHUNKS // 2 else 0

    def up_or_down(side):
        return {"ep": at["up"] if side == 1 else at["down"]}

    def sum_hop(s, side, h):
        src = moving.at[s, side, pl.ds(h * part, part)]
        dst = moving.at[s - 1, side, pl.ds(h * part, part)]
        return remote(src, dst, zs2.at[s - 1, side, h], zr2.at[s - 1, side, h], up_or_down(side))

    def first_sum(side, h):
        src = terms.at[0, 1, pl.ds(h * part, part)]
        dst = moving.at[pairs - 1, side, pl.ds(h * part, part)]
        return remote(src, dst, zs2.at[pairs - 1, side, h], zr2.at[pairs - 1, side, h], up_or_down(side))

    def far(p):
        return {"tp": at["right"] if p == 0 else at["left"]}

    def near(p):
        return {"tp": at["left"] if p == 0 else at["right"]}

    def two_away(t, p):
        return remote(parts.at[at["across"], t], across.at[t], xs2.at[t, 0], xr2.at[t, 0], far(p))

    def one_away(t, p):
        col = at["left"] if p == 0 else at["right"]
        return remote(parts.at[col, t], direct.at[t], xs2.at[t, 1], xr2.at[t, 1], near(p))

    def onward(t, p):
        return remote(staged.at[t], summed.at[t], xs2.at[t, 2], xr2.at[t, 2], far(p))

    def give(pos):
        return remote(given.at[pos], outs.at[pos, pl.ds(16, 16)], ds2.at[pos], dr2.at[pos], {"ep": at["pal"]})

    for h in range(CHUNKS):
        side = 1 - out_side(h)
        moving[pairs - 1, side, h * part : (h + 1) * part] = jnp.zeros((part, width), BF16)

    down_each = -(-tp // (half - 1)) if half > 1 else tp

    if half <= 1:
        for q in range(tp):
            project_down(q, 0)

    def scatter(t, carry):
        @pl.when(t < pairs)
        def _():
            pos = pairs - 1 - t
            for p in range(2):
                two_away(pos * 2 + p, p).start()
            for p in range(2):
                one_away(pos * 2 + p, p).start()

        @pl.when(t >= 7)
        def _():
            u = t - 7
            pair = lax.rem(pairs - u, pairs)

            @pl.when(u == 0)
            def _():
                for h in range(CHUNKS):
                    first_sum(out_side(h), h).start()

            @pl.when(u > 0)
            def _():
                for h in range(CHUNKS):
                    for side in (out_side(h), 1 - out_side(h)):
                        rows_at = pl.ds(h * part, part)
                        arrival = remote(
                            moving.at[pair, side, rows_at],
                            moving.at[pair, side, rows_at],
                            zs2.at[pair, side, h],
                            zr2.at[pair, side, h],
                            up_or_down(side),
                        )
                        if side == out_side(h):
                            arrival.wait_recv()
                        else:

                            @pl.when(u > 1)
                            def _():
                                arrival.wait_recv()

                        value = moving[pair, side, rows_at].astype(F32) + terms[pair, side, rows_at].astype(F32)
                        moving[pair, side, rows_at] = value.astype(BF16)
                        sum_hop(pair, side, h).start()

        @pl.when((t >= 6) & (t < pairs + 6))
        def _():
            pos = pairs + 5 - t
            pair = lax.rem(pos + 1, pairs)
            give(pos).wait_recv()
            mixed = dot(mix[pair][:, :32], outs[pos])
            terms[pair] = mixed.astype(BF16).reshape(2, tokens, width)

            @pl.when(t == 6)
            def _():
                own_sum[...] = mixed[:tokens]

        @pl.when((t >= 2) & (t < pairs + 2))
        def _():
            for p in range(2):
                t1 = (pairs + 1 - t) * 2 + p
                two_away(t1, p).wait_recv()
                col = at["right"] if p == 0 else at["left"]
                staged[t1] = (across[t1].astype(F32) + parts[col, t1].astype(F32)).astype(BF16)
                onward(t1, p).start()

        @pl.when((t >= 4) & (t < pairs + 4))
        def _():
            pos = pairs + 3 - t
            for p in (1, 0):
                t2 = pos * 2 + p
                one_away(t2, p).wait_recv()
                onward(t2, p).wait_recv()
                total = (
                    summed[t2].astype(F32)
                    + direct[t2].astype(F32)
                    + parts[at["col"], t2].astype(F32)
                    + down_bias[...]
                ).astype(BF16)
                if p == 1:
                    given[pos] = total
                    give(pos).start()
                else:
                    outs[pos, :16] = total

        if half > 1:
            for k in range(down_each):
                q = (t - 1) * down_each + k

                @pl.when((t >= 1) & (q < tp))
                def _():
                    project_down(q, 0)

        return carry

    lax.fori_loop(0, pairs + 7, scatter, 0)

    for side in range(2):
        for h in range(CHUNKS):
            sum_hop(1, side, h).wait_recv()
    total = own[...] + own_sum[...] + moving[0, 0].astype(F32) + moving[0, 1].astype(F32)
    out_ref[...] = total[:, : out_ref.shape[1]].astype(BF16)

    def finish(pos, carry):
        to_pal(pos).wait_send()
        give(pos).wait_send()
        for p in range(2):
            go_right(pos, p).wait_send()
            go_left(pos, p).wait_send()
            relay(pos, p).wait_send()
            two_away(pos * 2 + p, p).wait_send()
            one_away(pos * 2 + p, p).wait_send()
            onward(pos * 2 + p, p).wait_send()
        return carry

    lax.fori_loop(0, pairs, finish, 0)

    def sent(s, carry):
        for side in range(2):
            for h in range(CHUNKS):
                hop(s, side, h).wait_send()
                sum_hop(s, side, h).wait_send()
        return carry

    lax.fori_loop(1, pairs, sent, 0)
    for h in range(CHUNKS):
        last_hop(last_side(h), h).wait_send()
        first_sum(out_side(h), h).wait_send()


def layer(hidden, ids, weights, gain, codes, scales, up_bias, low_codes, low_scales, down_bias, ep, tp):
    tokens, model_width = hidden.shape
    top = ids.shape[1]
    quarter = model_width // tp
    width = -(-(quarter + 2 * top) // 128) * 128
    whole_width = -(-model_width // 128) * 128 + 128
    pairs = ep // 4
    word_rows, columns = codes.shape
    hidden_units = low_codes.shape[1]
    low_lanes = -(-low_codes.shape[0] // 128) * 128
    blocks = low_scales.shape[0]
    low_parts = max(1, pairs // tp)
    tiles = 2 * pairs
    dma = pltpu.SemaphoreType.DMA
    vmem = pl.BlockSpec(memory_space=pltpu.VMEM)
    hbm = pl.BlockSpec(memory_space=pl.ANY)
    ring = dma((pairs, 2, CHUNKS))
    return pl.pallas_call(
        functools.partial(layer_kernel, ep, tp, top, quarter - (width - 128)),
        out_shape=jax.ShapeDtypeStruct((tokens, quarter), BF16),
        in_specs=[vmem] * 4 + [hbm, hbm, vmem, hbm, hbm, vmem],
        out_specs=vmem,
        scratch_shapes=[
            pltpu.VMEM((low_lanes, hidden_units), jnp.int32),
            pltpu.VMEM((tokens, whole_width), F32),
            pltpu.VMEM((blocks, whole_width), F32),
            pltpu.VMEM((blocks, model_width), BF16),
            pltpu.VMEM((tp * low_parts, blocks // low_parts, width), F32),
            pltpu.VMEM((1, width), F32),
            pltpu.VMEM((tokens, width), F32),
            pltpu.VMEM((tokens, width), BF16),
            pltpu.VMEM((pairs, 2, tokens, width), BF16),
            pltpu.VMEM((pairs, 16, width), BF16),
            pltpu.VMEM((tp, tiles, 16, width), BF16),
            pltpu.VMEM((pairs, 2 * tokens, 128), BF16),
            pltpu.VMEM((word_rows, columns), jnp.int32),
            pltpu.VMEM(scales.shape, BF16),
            pltpu.VMEM(scales.shape, F32),
            pltpu.VMEM((hidden_units, low_lanes), jnp.int32),
            pltpu.VMEM((tp * width // 16, 16, columns), BF16),
            pltpu.VMEM((tp, hidden_units, width), BF16),
            pltpu.VMEM((1024, width), BF16),
            pltpu.VMEM((2, 16 * pairs, hidden_units), BF16),
            pltpu.VMEM((tp, tiles, 16, width), BF16),
            pltpu.VMEM((tiles, 16, width), BF16),
            pltpu.VMEM((tiles, 16, width), BF16),
            pltpu.VMEM((tiles, 16, width), BF16),
            pltpu.VMEM((tiles, 16, width), BF16),
            pltpu.VMEM((pairs, 32, width), BF16),
            pltpu.VMEM((pairs, 16, width), BF16),
            pltpu.VMEM((pairs, 2, tokens, width), BF16),
            pltpu.VMEM((pairs, 2, tokens, width), BF16),
            pltpu.VMEM((tokens, width), F32),
            dma((4,)),
            ring, ring, dma((pairs,)), dma((pairs,)), dma((tiles, 3)), dma((tiles, 3)),
            ring, ring, dma((pairs,)), dma((pairs,)), dma((tiles, 3)), dma((tiles, 3)),
        ],
        compiler_params=pltpu.CompilerParams(
            collective_id=0, has_side_effects=True, vmem_limit_bytes=60 << 20
        ),
        name="layer",
    )(hidden, ids, weights, gain, codes, scales, up_bias, low_codes, low_scales, down_bias)


def shards(
    hidden,
    route_experts,
    route_weight,
    norm_gain,
    gate_up_codes,
    gate_up_scales,
    gate_up_bias,
    down_codes,
    down_scales,
    down_bias,
):
    return layer(
        hidden,
        route_experts,
        route_weight,
        norm_gain[None],
        gate_up_codes[0],
        gate_up_scales[0],
        gate_up_bias,
        down_codes[0].T,
        down_scales[0],
        down_bias,
        lax.axis_size("ep"),
        lax.axis_size("tp"),
    )


def solution(mesh):
    placed = (
        P(("groups", "ep"), None),
        P(("groups", "ep"), None),
        P(("groups", "ep"), None),
        P(),
        P("ep", None, "tp"),
        P("ep", None, "tp"),
        P("ep", "tp"),
        P("ep", "tp", None),
        P("ep", "tp", None),
        P("ep", "tp"),
    )
    return jax.shard_map(
        shards, mesh=mesh, in_specs=placed, out_specs=P(("groups", "ep"), "tp"), check_vma=False
    )
```

```python
import functools

import jax
import jax.numpy as jnp
from jax import lax
from jax.experimental import pallas as pl
from jax.experimental.pallas import tpu as pltpu
from jax.sharding import PartitionSpec as P

CAP = 8
CHUNKS = 4
F32 = jnp.float32
BF16 = jnp.bfloat16


def dot(a, b):
    return jnp.dot(a, b, preferred_element_type=F32)


def iota(shape, dim):
    return lax.broadcasted_iota(jnp.int32, shape, dim)


def neighbours(ep, tp):
    me = lax.axis_index("ep")
    core = lax.rem(me, 2)
    col = lax.axis_index("tp")
    return dict(
        me=me,
        up=lax.rem(me + 3 - 2 * core, ep),
        down=lax.rem(me + ep - 1 - 2 * core, ep),
        pal=me + 1 - 2 * core,
        col=col,
        right=lax.rem(col + 1, tp),
        left=lax.rem(col + tp - 1, tp),
        across=lax.rem(col + 2, tp),
    )


def greet(at):
    barrier = pltpu.get_barrier_semaphore()
    for place in ({"ep": at["up"]}, {"ep": at["down"]}, {"ep": at["pal"]}, {"tp": at["right"]}, {"tp": at["left"]}):
        pl.semaphore_signal(barrier, inc=1, device_id=place, device_id_type=pl.DeviceIdType.MESH)
    return barrier


def remote(src, dst, send, recv, place):
    return pltpu.make_async_remote_copy(
        src_ref=src, dst_ref=dst, send_sem=send, recv_sem=recv, device_id=place, device_id_type=pl.DeviceIdType.MESH
    )


def nibble_value(word, shift):
    top_bits = lax.shift_left(word, 28 - shift)
    magnit = lax.shift_right_logical(top_bits, 28) & 7
    doubled = magnit + jnp.maximum(magnit - 4, 0) + 2 * jnp.maximum(magnit - 6, 0)
    value = doubled.astype(F32)
    return jnp.where(top_bits < 0, -value, value)


def layer_kernel(
    ep, tp, top, meta_at,
    hidden_ref, ids_ref, weights_ref, gain_ref, codes_hbm, scales_hbm, up_bias_ref, low_codes_hbm,
    low_scales_hbm, down_bias_ref,
    out_ref,
    turned_codes,    wide, wide_scales, narrow_scales, low_scales, down_bias, own, block_ref, held, handed, rows, mix,
    codes, scales, scales32, low_codes, upper, lower, spread, act, parts,
    across, summed, staged, direct, outs, given, moving, terms, own_sum,
    local_sem, zs, zr, ds, dr, xs, xr, zs2, zr2, ds2, dr2, xs2, xr2,
):
    pairs = held.shape[0]
    tokens = held.shape[2]
    width = held.shape[3]
    part = tokens // CHUNKS
    half = pairs // 2
    columns = codes.shape[1]
    hidden_units = lower.shape[1]
    units = upper.shape[0] // tp
    word_rows = codes.shape[0]
    real_units = word_rows // 2 // tp
    words = real_units * 2
    at = neighbours(ep, tp)
    barrier = greet(at)

    fetches = [
        pltpu.make_async_copy(codes_hbm, codes, local_sem.at[1]),
        pltpu.make_async_copy(scales_hbm, scales, local_sem.at[2]),
        pltpu.make_async_copy(low_codes_hbm, turned_codes.at[pl.ds(0, low_codes_hbm.shape[0])], local_sem.at[3]),
        pltpu.make_async_copy(low_scales_hbm, narrow_scales, local_sem.at[0]),
    ]
    for fetch in fetches:
        fetch.start()

    model_width = hidden_ref.shape[1]
    quarter = out_ref.shape[1]
    whole_width = wide.shape[1]
    rest = jnp.zeros((tokens, whole_width - model_width), F32)
    widened = hidden_ref[...].astype(F32)
    mean_square = jnp.mean(widened * widened, axis=-1, keepdims=True)
    back = lax.rem(whole_width - at["col"] * quarter, whole_width)
    wide[:, :model_width] = widened
    wide[:, model_width:] = rest
    own[...] = pltpu.roll(wide[...], back, axis=1)[:, :width]
    wide[:8, :model_width] = jnp.broadcast_to(gain_ref[...].astype(F32), (8, model_width))
    gain = pltpu.roll(wide[:8], back, axis=1)[:1, :width]
    normed = (own[...] * lax.rsqrt(mean_square + 1e-05) * gain).astype(BF16).astype(F32)
    choice, meta_lane = iota((top, 128), 0), iota((top, 128), 1)
    meta_own = dot(ids_ref[...].astype(F32).astype(BF16), (meta_lane == meta_at + choice).astype(BF16))
    meta_own = meta_own + dot(
        weights_ref[...].astype(BF16), (meta_lane == meta_at + top + choice).astype(BF16)
    )
    if width > 128:
        block_ref[:, : width - 128] = normed[:, : width - 128].astype(BF16)
    is_data = iota((tokens, 128), 1) < meta_at
    block_ref[:, width - 128 :] = jnp.where(is_data, normed[:, width - 128 :], meta_own).astype(BF16)
    pl.semaphore_wait(barrier, 5)

    def piece(pair, side, h):
        return held.at[pair, side, pl.ds(h * part, part)]

    def hop(s, side, h):
        src = piece(s - 1, side, h)
        if isinstance(s, int) and s == 1:
            src = block_ref.at[pl.ds(h * part, part)]
        place = {"ep": at["up"] if side == 0 else at["down"]}
        return remote(src, piece(s, side, h), zs.at[s, side, h], zr.at[s, side, h], place)

    def last_hop(side, h):
        place = {"ep": at["up"] if side == 0 else at["down"]}
        return remote(
            piece(pairs - 1, side, h), piece(0, 1, h), zs.at[0, side, h], zr.at[0, side, h], place
        )

    def last_side(h):
        return 0 if h < CHUNKS // 2 else 1

    def tile(col, pos, p):
        return rows.at[col, pos * 2 + p]

    def to_pal(pos):
        return remote(handed.at[pos], tile(at["col"], pos, 1), ds.at[pos], dr.at[pos], {"ep": at["pal"]})

    def x_copy(col, pos, p, kind, place):
        return remote(
            tile(col, pos, p), tile(col, pos, p), xs.at[pos * 2 + p, kind], xr.at[pos * 2 + p, kind],
            {"tp": place},
        )

    def go_right(pos, p):
        return x_copy(at["col"], pos, p, 0, at["right"])

    def go_left(pos, p):
        return x_copy(at["col"], pos, p, 1, at["left"])

    def from_left(pos, p):
        return x_copy(at["left"], pos, p, 0, at["right"])

    def from_right(pos, p):
        return x_copy(at["right"], pos, p, 1, at["left"])

    def relay(pos, p):
        if p == 0:
            return x_copy(at["left"], pos, p, 2, at["right"])
        return x_copy(at["right"], pos, p, 2, at["left"])

    def relayed(pos, p):
        return x_copy(at["across"], pos, p, 2, at["right"])

    for h in range(CHUNKS):
        for side in range(2):
            hop(1, side, h).start()
    held[0, 0] = block_ref[...]

    both = 2 * tokens
    lane = iota((both, 128), 1)
    ls = iota((128, 128), 1)
    own_cols = (ls < 16).astype(BF16)
    pal_cols = ((ls >= 16) & (ls < 32)).astype(BF16)
    ti, tj = iota((both, both), 0), iota((both, both), 1)
    earlier = ((tj < ti) & ((ti < tokens) == (tj < tokens))).astype(BF16)
    wanted = (lax.rem(lane, 16) - jnp.where(iota((both, 128), 0) >= tokens, 8, 0)).astype(F32)
    id_lanes = (lane >= meta_at) & (lane < meta_at + top)
    own_id = at["me"].astype(F32)
    pal_id = at["pal"].astype(F32)

    def select(pair, pos):
        block = held[pair].reshape(both, width)
        meta = block[:, width - 128 :].astype(F32)
        weights = pltpu.roll(meta, 128 - top, axis=1)
        is_own = id_lanes & (meta == own_id)
        is_pal = id_lanes & (meta == pal_id)
        match = dot(jnp.where(is_own, 1.0, 0.0).astype(BF16), own_cols) + dot(
            jnp.where(is_pal, 1.0, 0.0).astype(BF16), pal_cols
        )
        weight = dot(jnp.where(is_own, weights, 0.0).astype(BF16), own_cols) + dot(
            jnp.where(is_pal, weights, 0.0).astype(BF16), pal_cols
        )
        slot = dot(earlier, match.astype(BF16))
        placed = (match > 0.5) & (slot == wanted)
        mix[pair] = jnp.where(placed, weight, 0.0).astype(BF16)
        pick = jnp.transpose(jnp.where(placed, 1.0, 0.0))[:32].astype(BF16)
        picked = dot(pick, block).astype(BF16)
        rows[at["col"], pos * 2] = picked[:16]
        handed[pos] = picked[16:]

    for q in range(tp):
        upper[q * units + real_units : (q + 1) * units] = jnp.zeros((units - real_units, 16, columns), BF16)
    word, lanes = iota((128, width), 0), iota((128, width), 1)
    for j in range(8):
        spread[j * 128 : (j + 1) * 128] = (lanes == 8 * word + j).astype(BF16)
    for fetch in fetches:
        fetch.wait()
    turned_codes[words * tp :] = jnp.zeros((turned_codes.shape[0] - words * tp, hidden_units), jnp.int32)
    low_codes[...] = jnp.transpose(turned_codes[...])
    scales32[...] = 0.5 * scales[...].astype(F32)
    low_parts = max(1, pairs // tp)
    blocks = wide_scales.shape[0]
    each = blocks // low_parts
    wide_scales[:, :model_width] = 0.5 * narrow_scales[...].astype(F32)
    wide_scales[:, model_width:] = jnp.zeros((blocks, whole_width - model_width), F32)
    for q in range(tp):
        turned = wide_scales[...]
        if q:
            turned = pltpu.roll(turned, whole_width - q * quarter, axis=1)
        turned = jnp.where(iota((blocks, width), 1) < quarter, turned[:, :width], 0.0)
        for r in range(low_parts):
            low_scales[q * low_parts + r] = turned[r * each : (r + 1) * each]
    down_bias[...] = jnp.zeros_like(down_bias)
    down_bias[:, :quarter] = down_bias_ref[...].astype(F32)

    def decode(u):
        packed = codes[pl.ds(pl.multiple_of(u * 8, 8), 8), :]
        shift = 4 * iota((8, 8, columns), 1)
        value = nibble_value(jnp.broadcast_to(packed[:, None, :], (8, 8, columns)), shift)
        value = value.reshape(2, 32, columns)
        for k in range(2):
            scaled = (value[k] * scales32[pl.ds(2 * u + k, 1), :]).astype(BF16).reshape(2, 16, columns)
            for m in range(2):
                unit = 4 * u + 2 * k + m
                upper[unit + (units - real_units) * (unit // real_units)] = scaled[m]

    low_rows = hidden_units // low_parts
    low_each = tp * low_parts // pairs
    low_lanes = low_codes.shape[1]
    window = min(256, low_lanes)

    def decode_low(i):
        q, r = i // low_parts, lax.rem(i, low_parts)
        begin = jnp.minimum(128 * ((words * q) // 128), low_lanes - window)
        packed = low_codes[
            pl.ds(pl.multiple_of(r * low_rows, 32), low_rows), pl.ds(pl.multiple_of(begin, 128), window)
        ]
        packed = pltpu.roll(packed, lax.rem(window + begin - words * q, window), axis=1)[:, :128]
        whole = jnp.concatenate([nibble_value(packed, 4 * j).astype(BF16) for j in range(8)], axis=1)
        value = dot(whole, spread[...]).reshape(low_rows // 32, 32, width)
        value = value * low_scales[i][:, None, :]
        lower[q, pl.ds(pl.multiple_of(r * low_rows, 32), low_rows)] = value.reshape(low_rows, width).astype(BF16)

    tiles_n = columns // 256
    si, sj = iota((256, 128), 0), iota((256, 128), 1)
    evens = (si == 2 * sj).astype(BF16)

    def project(n, part_at):
        at_n = pl.ds(pl.multiple_of(n * 256, 256), 256)
        total = jnp.broadcast_to(up_bias_ref[:, at_n].astype(F32), (16 * pairs, 256))
        for q in range(tp):
            weight = upper[q * units : (q + 1) * units, :, at_n].reshape(units * 16, 256)
            given_rows = rows[q, part_at * pairs : (part_at + 1) * pairs].reshape(16 * pairs, width)
            total = total + dot(given_rows, weight)
        gate = jnp.minimum(total, 7.0)
        upward = jnp.clip(pltpu.roll(total, 255, axis=1), -7.0, 7.0)
        value = (gate * jax.nn.sigmoid(1.702 * gate) * (upward + 1.0)).astype(BF16)
        act[part_at, :, pl.ds(pl.multiple_of(n * 128, 128), 128)] = dot(value, evens).astype(BF16)

    def project_down(q, part_at):
        value = dot(act[part_at], lower[q]).astype(BF16)
        parts[q, part_at * pairs : (part_at + 1) * pairs] = value.reshape(pairs, 16, width)

    lag = 2
    project_from = half + 2 * lag + 1
    projected = max(0, min(tiles_n, pairs + 2 * lag - project_from))
    decodes = word_rows // 8
    per_step = -(-decodes // min(pairs - 1, project_from))
    decode_steps = -(-decodes // per_step)

    def arrive(pos, carry):
        from_right(pos, 0).wait_recv()
        from_left(pos, 1).wait_recv()
        for p in range(2):
            relayed(pos, p).wait_recv()
        return carry

    def x_action(i, u):
        if i < 2:

            @pl.when((u >= 1) & (u < pairs + 1))
            def _():
                (go_right if i == 0 else go_left)(u - 1, 0).start()

        elif i < 4:

            @pl.when((u >= 2) & (u < pairs + 2))
            def _():
                if i == 2:
                    to_pal(u - 2).wait_recv()
                (go_right if i == 2 else go_left)(u - 2, 1).start()

        elif i == 4:

            @pl.when((u >= 3) & (u < pairs + 3))
            def _():
                from_left(u - 3, 0).wait_recv()
                relay(u - 3, 0).start()

        else:

            @pl.when(u >= 4)
            def _():
                from_right(u - 4, 1).wait_recv()
                relay(u - 4, 1).start()

    def spread_out(n, count):
        return range(count * n // (2 * CHUNKS), count * (n + 1) // (2 * CHUNKS))

    def gather(u, carry):
        @pl.when(u < pairs - 1)
        def _():
            s = u + 1
            for h in range(CHUNKS):
                for side in range(2):
                    hop(s, side, h).wait_recv()

                    @pl.when(s < pairs - 1)
                    def _():
                        hop(s + 1, side, h).start()

                    if side == last_side(h):

                        @pl.when(s == pairs - 1)
                        def _():
                            last_hop(side, h).start()

                    for i in spread_out(2 * h + side, 6):
                        x_action(i, u)

        @pl.when(u >= pairs - 1)
        def _():
            for i in range(6):
                x_action(i, u)

        @pl.when(u == pairs - 1)
        def _():
            for h in range(CHUNKS):
                last_hop(last_side(h), h).wait_recv()

        @pl.when(u < decode_steps)
        def _():
            for k in range(per_step):
                if per_step * decode_steps == decodes:
                    decode(u * per_step + k)
                else:

                    @pl.when(u * per_step + k < decodes)
                    def _():
                        decode(u * per_step + k)

        @pl.when(u < pairs)
        def _():
            select(lax.rem(u + 1, pairs), u)
            to_pal(u).start()

        @pl.when(u < pairs)
        def _():
            for k in range(low_each):
                decode_low(u * low_each + k)

        if projected:

            @pl.when(u == project_from)
            def _():
                lax.fori_loop(0, half, arrive, 0)

            @pl.when((u >= project_from) & (u < project_from + projected))
            def _():
                project(u - project_from, 0)

        return carry

    lax.fori_loop(0, pairs + 2 * lag, gather, 0)
    lax.fori_loop(half if projected else 0, pairs, arrive, 0)

    def project_rest(n, carry):
        project(n, 0)
        return carry

    def project_late(n, carry):
        project(n, 1)
        return carry

    def down_late(q, carry):
        project_down(q, 1)
        return carry

    if projected < tiles_n:
        lax.fori_loop(projected, tiles_n, project_rest, 0)
    lax.fori_loop(0, tiles_n, project_late, 0)
    lax.fori_loop(0, tp, down_late, 0)

    def out_side(h):
        return 1 if h < CHUNKS // 2 else 0

    def up_or_down(side):
        return {"ep": at["up"] if side == 1 else at["down"]}

    def sum_hop(s, side, h):
        src = moving.at[s, side, pl.ds(h * part, part)]
        dst = moving.at[s - 1, side, pl.ds(h * part, part)]
        return remote(src, dst, zs2.at[s - 1, side, h], zr2.at[s - 1, side, h], up_or_down(side))

    def first_sum(side, h):
        src = terms.at[0, 1, pl.ds(h * part, part)]
        dst = moving.at[pairs - 1, side, pl.ds(h * part, part)]
        return remote(src, dst, zs2.at[pairs - 1, side, h], zr2.at[pairs - 1, side, h], up_or_down(side))

    def far(p):
        return {"tp": at["right"] if p == 0 else at["left"]}

    def near(p):
        return {"tp": at["left"] if p == 0 else at["right"]}

    def two_away(t, p):
        return remote(parts.at[at["across"], t], across.at[t], xs2.at[t, 0], xr2.at[t, 0], far(p))

    def one_away(t, p):
        col = at["left"] if p == 0 else at["right"]
        return remote(parts.at[col, t], direct.at[t], xs2.at[t, 1], xr2.at[t, 1], near(p))

    def onward(t, p):
        return remote(staged.at[t], summed.at[t], xs2.at[t, 2], xr2.at[t, 2], far(p))

    def give(pos):
        return remote(given.at[pos], outs.at[pos, pl.ds(16, 16)], ds2.at[pos], dr2.at[pos], {"ep": at["pal"]})

    for h in range(CHUNKS):
        side = 1 - out_side(h)
        moving[pairs - 1, side, h * part : (h + 1) * part] = jnp.zeros((part, width), BF16)

    down_each = -(-tp // (half - 1)) if half > 1 else tp

    if half <= 1:
        for q in range(tp):
            project_down(q, 0)

    def sum_action(i, t):
        if i < 4:

            @pl.when(t < pairs)
            def _():
                p = i % 2
                (two_away if i < 2 else one_away)((pairs - 1 - t) * 2 + p, p).start()

        else:

            @pl.when((t >= 2) & (t < pairs + 2))
            def _():
                p = i - 4
                t1 = (pairs + 1 - t) * 2 + p
                two_away(t1, p).wait_recv()
                col = at["right"] if p == 0 else at["left"]
                staged[t1] = (across[t1].astype(F32) + parts[col, t1].astype(F32)).astype(BF16)
                onward(t1, p).start()

    def scatter(t, carry):
        @pl.when(t >= 7)
        def _():
            u = t - 7
            pair = lax.rem(pairs - u, pairs)

            @pl.when(u == 0)
            def _():
                for h in range(CHUNKS):
                    first_sum(out_side(h), h).start()

            @pl.when(u > 0)
            def _():
                for h in range(CHUNKS):
                    for side in (out_side(h), 1 - out_side(h)):
                        rows_at = pl.ds(h * part, part)
                        arrival = remote(
                            moving.at[pair, side, rows_at],
                            moving.at[pair, side, rows_at],
                            zs2.at[pair, side, h],
                            zr2.at[pair, side, h],
                            up_or_down(side),
                        )
                        if side == out_side(h):
                            arrival.wait_recv()
                        else:

                            @pl.when(u > 1)
                            def _():
                                arrival.wait_recv()

                        value = moving[pair, side, rows_at].astype(F32) + terms[pair, side, rows_at].astype(F32)
                        moving[pair, side, rows_at] = value.astype(BF16)
                        sum_hop(pair, side, h).start()
                        for i in spread_out(2 * h + (side != out_side(h)), 6):
                            sum_action(i, t)

        @pl.when(t < 8)
        def _():
            for i in range(6):
                sum_action(i, t)

        @pl.when((t >= 6) & (t < pairs + 6))
        def _():
            pos = pairs + 5 - t
            pair = lax.rem(pos + 1, pairs)
            give(pos).wait_recv()
            mixed = dot(mix[pair][:, :32], outs[pos])
            terms[pair] = mixed.astype(BF16).reshape(2, tokens, width)

            @pl.when(t == 6)
            def _():
                own_sum[...] = mixed[:tokens]

        @pl.when((t >= 4) & (t < pairs + 4))
        def _():
            pos = pairs + 3 - t
            for p in (1, 0):
                t2 = pos * 2 + p
                one_away(t2, p).wait_recv()
                onward(t2, p).wait_recv()
                total = (
                    summed[t2].astype(F32)
                    + direct[t2].astype(F32)
                    + parts[at["col"], t2].astype(F32)
                    + down_bias[...]
                ).astype(BF16)
                if p == 1:
                    given[pos] = total
                    give(pos).start()
                else:
                    outs[pos, :16] = total

        if half > 1:
            for k in range(down_each):
                q = (t - 1) * down_each + k

                @pl.when((t >= 1) & (q < tp))
                def _():
                    project_down(q, 0)

        return carry

    lax.fori_loop(0, pairs + 7, scatter, 0)

    for side in range(2):
        for h in range(CHUNKS):
            sum_hop(1, side, h).wait_recv()
    total = own[...] + own_sum[...] + moving[0, 0].astype(F32) + moving[0, 1].astype(F32)
    out_ref[...] = total[:, : out_ref.shape[1]].astype(BF16)

    def finish(pos, carry):
        to_pal(pos).wait_send()
        give(pos).wait_send()
        for p in range(2):
            go_right(pos, p).wait_send()
            go_left(pos, p).wait_send()
            relay(pos, p).wait_send()
            two_away(pos * 2 + p, p).wait_send()
            one_away(pos * 2 + p, p).wait_send()
            onward(pos * 2 + p, p).wait_send()
        return carry

    lax.fori_loop(0, pairs, finish, 0)

    def sent(s, carry):
        for side in range(2):
            for h in range(CHUNKS):
                hop(s, side, h).wait_send()
                sum_hop(s, side, h).wait_send()
        return carry

    lax.fori_loop(1, pairs, sent, 0)
    for h in range(CHUNKS):
        last_hop(last_side(h), h).wait_send()
        first_sum(out_side(h), h).wait_send()


def layer(hidden, ids, weights, gain, codes, scales, up_bias, low_codes, low_scales, down_bias, ep, tp):
    tokens, model_width = hidden.shape
    top = ids.shape[1]
    quarter = model_width // tp
    width = -(-(quarter + 2 * top) // 128) * 128
    whole_width = -(-model_width // 128) * 128 + 128
    pairs = ep // 4
    word_rows, columns = codes.shape
    hidden_units = low_codes.shape[1]
    low_lanes = -(-low_codes.shape[0] // 128) * 128
    blocks = low_scales.shape[0]
    low_parts = max(1, pairs // tp)
    tiles = 2 * pairs
    dma = pltpu.SemaphoreType.DMA
    vmem = pl.BlockSpec(memory_space=pltpu.VMEM)
    hbm = pl.BlockSpec(memory_space=pl.ANY)
    ring = dma((pairs, 2, CHUNKS))
    return pl.pallas_call(
        functools.partial(layer_kernel, ep, tp, top, quarter - (width - 128)),
        out_shape=jax.ShapeDtypeStruct((tokens, quarter), BF16),
        in_specs=[vmem] * 4 + [hbm, hbm, vmem, hbm, hbm, vmem],
        out_specs=vmem,
        scratch_shapes=[
            pltpu.VMEM((low_lanes, hidden_units), jnp.int32),
            pltpu.VMEM((tokens, whole_width), F32),
            pltpu.VMEM((blocks, whole_width), F32),
            pltpu.VMEM((blocks, model_width), BF16),
            pltpu.VMEM((tp * low_parts, blocks // low_parts, width), F32),
            pltpu.VMEM((1, width), F32),
            pltpu.VMEM((tokens, width), F32),
            pltpu.VMEM((tokens, width), BF16),
            pltpu.VMEM((pairs, 2, tokens, width), BF16),
            pltpu.VMEM((pairs, 16, width), BF16),
            pltpu.VMEM((tp, tiles, 16, width), BF16),
            pltpu.VMEM((pairs, 2 * tokens, 128), BF16),
            pltpu.VMEM((word_rows, columns), jnp.int32),
            pltpu.VMEM(scales.shape, BF16),
            pltpu.VMEM(scales.shape, F32),
            pltpu.VMEM((hidden_units, low_lanes), jnp.int32),
            pltpu.VMEM((tp * width // 16, 16, columns), BF16),
            pltpu.VMEM((tp, hidden_units, width), BF16),
            pltpu.VMEM((1024, width), BF16),
            pltpu.VMEM((2, 16 * pairs, hidden_units), BF16),
            pltpu.VMEM((tp, tiles, 16, width), BF16),
            pltpu.VMEM((tiles, 16, width), BF16),
            pltpu.VMEM((tiles, 16, width), BF16),
            pltpu.VMEM((tiles, 16, width), BF16),
            pltpu.VMEM((tiles, 16, width), BF16),
            pltpu.VMEM((pairs, 32, width), BF16),
            pltpu.VMEM((pairs, 16, width), BF16),
            pltpu.VMEM((pairs, 2, tokens, width), BF16),
            pltpu.VMEM((pairs, 2, tokens, width), BF16),
            pltpu.VMEM((tokens, width), F32),
            dma((4,)),
            ring, ring, dma((pairs,)), dma((pairs,)), dma((tiles, 3)), dma((tiles, 3)),
            ring, ring, dma((pairs,)), dma((pairs,)), dma((tiles, 3)), dma((tiles, 3)),
        ],
        compiler_params=pltpu.CompilerParams(
            collective_id=0, has_side_effects=True, vmem_limit_bytes=60 << 20
        ),
        name="layer",
    )(hidden, ids, weights, gain, codes, scales, up_bias, low_codes, low_scales, down_bias)


def shards(
    hidden,
    route_experts,
    route_weight,
    norm_gain,
    gate_up_codes,
    gate_up_scales,
    gate_up_bias,
    down_codes,
    down_scales,
    down_bias,
):
    return layer(
        hidden,
        route_experts,
        route_weight,
        norm_gain[None],
        gate_up_codes[0],
        gate_up_scales[0],
        gate_up_bias,
        down_codes[0].T,
        down_scales[0],
        down_bias,
        lax.axis_size("ep"),
        lax.axis_size("tp"),
    )


def solution(mesh):
    placed = (
        P(("groups", "ep"), None),
        P(("groups", "ep"), None),
        P(("groups", "ep"), None),
        P(),
        P("ep", None, "tp"),
        P("ep", None, "tp"),
        P("ep", "tp"),
        P("ep", "tp", None),
        P("ep", "tp", None),
        P("ep", "tp"),
    )
    return jax.shard_map(
        shards, mesh=mesh, in_specs=placed, out_specs=P(("groups", "ep"), "tp"), check_vma=False
    )
```
